256 devices in a mesh: gx: 16 (over y, z_hi, core), gy: 4 (over z_lo), gz: 4 (over x).
Axes of the slice: x: 4, y: 4, z: 8 (z_hi: 2, z_lo: 4; z = z_hi * 4 + z_lo), core: 2. Of those that a mesh axis runs over, the one named last changes fastest.
Arguments:
- atom_cell: int32 [3, 65536], P(None, ('gx', 'gy', 'gz')), may hold values from 0 to 63, as said below
- atom_frac: bfloat16 [3, 65536], P(None, ('gx', 'gy', 'gz')), may hold values from 0 to 1
- features: bfloat16 [128, 65536], P(None, ('gx', 'gy', 'gz')), may hold values from -6 to 6
- ghost_export: int32 [16384], P(('gx', 'gy', 'gz')), may hold values from 0 to 255, as said below
- neighbors: int32 [65536, 32], P(('gx', 'gy', 'gz')), may hold values from 0 to 1983, as said below
- neighbor_count: int32 [65536], P(('gx', 'gy', 'gz')), may hold values from 16 to 32
- w_up: bfloat16 [128, 128], replicated, may hold values from -0.5 to 0.5
- radial_weight: float32 [128, 8], replicated, may hold values from -2 to 2
- w_out: bfloat16 [128, 128], replicated, may hold values from -0.5 to 0.5
- energy_weight: bfloat16 [128], replicated, may hold values from -0.5 to 0.5
- charge_weight: bfloat16 [128], replicated, may hold values from -0.5 to 0.5
Outputs:
- forces: float32 [3, 65536], P(None, ('gx', 'gy', 'gz'))
- atom_energy: float32 [65536], P(('gx', 'gy', 'gz'))
The draws below stay inside these ranges and needn't reach their ends.
Inputs may be any that keep to these rules, and one draw needn't show every extreme that they name: `atom_cell`: every atom whose cell is the first or one of the last two along some dimension of its domain is in its domain's ghost_export list. `ghost_export`: 64 distinct local atom indices of each domain. `neighbors`: each row names distinct entries of its domain's table, never the atom itself and never slot 13. Only the first neighbor_count entries of a row are neighbours.
All inputs are finite; a program needn't handle non-finite values.
Results may differ from the reference program's by a relative error of at most 0.0025.
Values may be sent and summed in bfloat16 or wider, within the bound.
A program may use at most 64 MiB of HBM per device.

```python
import math
import jax
import jax.numpy as jnp
from jax import lax

CHANNELS = 128
RADIAL = 8
NEIGHBORS = 32
BLOCK = 128
CX = 8
CY = 16
CZ = 64
ATOM_DEV = 256
EXPORT_DEV = 64
ATOMS = 65536
GX = 128
GY = 64
GZ = 256
N_GX = 16
N_GY = 4
N_GZ = 4


def shuffle_atoms(sub_key):
    return jax.random.permutation(sub_key, ATOM_DEV)


def atom_layout(key):
    count_x = GX // CX
    count_y = GY // CY
    count_z = GZ // CZ
    device_count = count_x * count_y * count_z
    base_key = jax.random.fold_in(key, 911)
    order_key, free_key, inner_key = jax.random.split(base_key, 3)
    orders = jax.vmap(shuffle_atoms)(jax.random.split(order_key, device_count)).astype(jnp.int32)
    export = orders[:, :EXPORT_DEV]
    ranks = jnp.argsort(orders, axis=1, stable=True)
    free_atom = ranks < EXPORT_DEV
    extents = jnp.array([CX, CY, CZ], jnp.int32)
    free_cells = jax.random.randint(free_key, (3, device_count, ATOM_DEV), 0, extents[:, None, None])
    inner_cells = jax.random.randint(inner_key, (3, device_count, ATOM_DEV), 1, extents[:, None, None] - 2)
    cells = jnp.where(free_atom[None], free_cells, inner_cells).astype(jnp.int32)
    return (cells, export.astype(jnp.int32))


def draw_atom_cell(key, part):
    cells, export = atom_layout(key)
    return cells.reshape(3, -1)


def draw_ghost_export(key, part):
    cells, export = atom_layout(key)
    return export.reshape(-1)


def draw_neighbors(key, part):
    cells, export = atom_layout(key)
    count_x = GX // CX
    count_y = GY // CY
    count_z = GZ // CZ
    device_count = count_x * count_y * count_z
    table_rows = ATOM_DEV + 27 * EXPORT_DEV
    devices = jnp.arange(device_count, dtype=jnp.int32)
    coord_x = devices // (count_y * count_z)
    coord_y = devices // count_z % count_y
    coord_z = devices % count_z
    slot_index = jnp.arange(27, dtype=jnp.int32)
    step_x = slot_index // 9 - 1
    step_y = slot_index // 3 % 3 - 1
    step_z = slot_index % 3 - 1
    partner = ((coord_x[:, None] + step_x[None]) % count_x * count_y + (coord_y[:, None] + step_y[None]) % count_y) * count_z + (coord_z[:, None] + step_z[None]) % count_z
    ghost_cells = cells[:, partner[:, :, None], export[partner]]
    slot_shift = jnp.stack([step_x * CX, step_y * CY, step_z * CZ])
    ghost_cells = ghost_cells + slot_shift[:, None, :, None]
    table = jnp.concatenate([cells, ghost_cells.reshape(3, device_count, 27 * EXPORT_DEV)], axis=2)
    salt_key = jax.random.fold_in(jax.random.fold_in(key, 911), 5)
    salts = jax.random.randint(salt_key, (device_count, ATOM_DEV), 0, table_rows)
    column = jnp.arange(table_rows, dtype=jnp.int32)
    blocked = jnp.logical_and(column >= ATOM_DEV + 13 * EXPORT_DEV, column < ATOM_DEV + 14 * EXPORT_DEV)

    def choose(device):
        own_cells = table[:, device, :ATOM_DEV]
        candidates = table[:, device, :]
        offsets = own_cells[:, :, None] - candidates[:, None, :]
        distance_sq = jnp.sum(offsets * offsets, axis=0)
        noise = (column[None, :] * 7919 + salts[device][:, None]) % table_rows
        score = distance_sq * table_rows + noise
        self_hit = column[None, :] == jnp.arange(ATOM_DEV, dtype=jnp.int32)[:, None]
        score = jnp.where(jnp.logical_or(self_hit, blocked[None, :]), 2 ** 30, score)
        return lax.top_k(-score, NEIGHBORS)[1]
    chosen = lax.map(choose, devices)
    return chosen.reshape(device_count * ATOM_DEV, NEIGHBORS).astype(jnp.int32)


def touch_ends(entries, own_key, low, high):
    shape = entries.shape
    place = [jax.random.randint(jax.random.fold_in(own_key, axis), (), 0, shape[axis]) for axis in range(len(shape))]
    entries = entries.at[tuple(place)].set(low)
    longest = shape.index(max(shape))
    place[longest] = (place[longest] + 1) % shape[longest]
    return entries.at[tuple(place)].set(high)


def steps_of(own_key, shape, shards, smallest, largest):
    gain = 1.0
    for dim, blocks in shards:
        heights = jax.random.uniform(jax.random.fold_in(jax.random.fold_in(own_key, 6), dim), (blocks,), jnp.float32, smallest / len(shards), largest / len(shards))
        gain = gain * jnp.repeat(jnp.exp(heights), shape[dim] // blocks).reshape((-1,) + (1,) * (len(shape) - 1 - dim))
    return gain


def bell_draw(rng, shape, spread, most, shards=(), kind=jnp.bfloat16):
    gain = steps_of(rng, shape, shards, -0.22, 0.18) if shards else 1.0
    result = jax.random.normal(rng, shape, jnp.float32) * spread * gain
    return jnp.minimum(jnp.maximum(result, -most), most).astype(kind)


def setup_inputs(seed: int = 0) -> dict:
    streams_of = jax.random.split(jax.random.key(seed), 12)
    return {
        "atom_cell": draw_atom_cell(jax.random.fold_in(streams_of[11], 71), 0),
        "atom_frac": jnp.clip(1.0 * jax.random.uniform(streams_of[1], (3, ATOMS), jnp.float32) ** steps_of(streams_of[1], (3, ATOMS), ((1, 256),), -0.2, 0.2), 0.0, 1.0).astype(jnp.bfloat16),
        "features": bell_draw(streams_of[2], (CHANNELS, ATOMS), 1.0, 6.0, ((1, 256),)),
        "ghost_export": draw_ghost_export(jax.random.fold_in(streams_of[11], 71), 0),
        "neighbors": draw_neighbors(jax.random.fold_in(streams_of[11], 71), 0),
        "neighbor_count": touch_ends(jax.random.randint(streams_of[5], (ATOMS,), NEIGHBORS // 2, NEIGHBORS + 1), jax.random.fold_in(streams_of[5], 1), NEIGHBORS // 2, NEIGHBORS).astype(jnp.int32),
        "w_up": bell_draw(streams_of[6], (CHANNELS, CHANNELS), CHANNELS ** -0.5, 0.5),
        "radial_weight": bell_draw(streams_of[7], (CHANNELS, RADIAL), RADIAL ** -0.5, 2.0, (), jnp.float32),
        "w_out": bell_draw(streams_of[8], (CHANNELS, CHANNELS), CHANNELS ** -0.5, 0.5),
        "energy_weight": bell_draw(streams_of[9], (CHANNELS,), CHANNELS ** -0.5, 0.5),
        "charge_weight": bell_draw(streams_of[10], (CHANNELS,), CHANNELS ** -0.5, 0.5),
    }


basis_step = 1.4
basis_width = 1.4
message_scale = 0.125
vector_scale = 1.0 / 6.0
ewald_beta_sq = 2.0

def spline_weights(fraction):
    remain = 1.0 - fraction
    squared = fraction * fraction
    cubed = squared * fraction
    return (remain * remain * remain / 6.0, (3.0 * cubed - 6.0 * squared + 4.0) / 6.0, (-3.0 * cubed + 3.0 * squared + 3.0 * fraction + 1.0) / 6.0, cubed / 6.0)

def block_energy(pos_table, up_table, centre_pos, centre_feat, neighbor_block, count_block, radial_weight, w_out, energy_weight):
    row_slots = neighbor_block.shape[1]
    atoms_block = neighbor_block.shape[0]
    flat_index = neighbor_block.T.reshape(-1)
    partner_pos = jnp.take(pos_table, flat_index, axis=1).reshape(3, row_slots, atoms_block)
    relative = partner_pos - centre_pos[:, None, :]
    distance = jnp.sqrt(lax.optimization_barrier(jnp.sum(relative * relative, axis=0)) + 1.0)
    valid_mask = (jnp.arange(row_slots)[:, None] < count_block[None, :]).astype(jnp.float32)
    centres = jnp.arange(radial_weight.shape[1]).astype(jnp.float32) * basis_step
    basis_values = jnp.exp(-jnp.square((distance[None] - centres[:, None, None]) / basis_width)) * valid_mask[None]
    radial = jnp.dot(radial_weight, basis_values.reshape(basis_values.shape[0], -1), precision=lax.Precision.HIGHEST, preferred_element_type=jnp.float32).reshape(-1, row_slots, atoms_block)
    partner_feat = jnp.take(up_table, flat_index, axis=1).reshape(-1, row_slots, atoms_block)
    message = radial * partner_feat.astype(jnp.float32)
    scalar = lax.optimization_barrier(jnp.sum(message, axis=1)) * message_scale
    vector = jnp.einsum('ckn,akn->acn', message, relative, precision=lax.Precision.HIGHEST) * (message_scale * vector_scale)
    invariant = scalar + scalar * scalar + lax.optimization_barrier(jnp.sum(vector * vector, axis=0))
    update = jnp.dot(w_out, invariant.astype(jnp.bfloat16), preferred_element_type=jnp.float32)
    hidden = centre_feat.astype(jnp.float32) + update
    return lax.optimization_barrier(jnp.sum(energy_weight.astype(jnp.float32)[:, None] * jax.nn.silu(hidden), axis=0))

def wave_number(indices, extent):
    folded = (indices + extent // 2) % extent - extent // 2
    return folded.astype(jnp.float32) * (2.0 * math.pi / extent)

def influence_of(wave_x, wave_y, wave_z, cells_total):
    square = wave_x[:, None, None] ** 2 + wave_y[None, :, None] ** 2 + wave_z[None, None, :] ** 2
    positive = square > 0.0
    safe_square = jnp.where(positive, square, 1.0)
    return jnp.where(positive, 4.0 * math.pi / cells_total * jnp.exp(-square / (4.0 * ewald_beta_sq)) / safe_square, 0.0)

def reference(atom_cell, atom_frac, features, ghost_export, neighbors, neighbor_count, w_up, radial_weight, w_out, energy_weight, charge_weight):
    device_count = N_GX * N_GY * N_GZ
    per_device = ATOM_DEV
    exported = EXPORT_DEV
    devices = jnp.arange(device_count, dtype=jnp.int32)
    coord_x = devices // (N_GY * N_GZ)
    coord_y = devices // N_GZ % N_GY
    coord_z = devices % N_GZ
    slot_index = jnp.arange(27, dtype=jnp.int32)
    step_x = slot_index // 9 - 1
    step_y = slot_index // 3 % 3 - 1
    step_z = slot_index % 3 - 1
    partner_device = ((coord_x[:, None] + step_x[None]) % N_GX * N_GY + (coord_y[:, None] + step_y[None]) % N_GY) * N_GZ + (coord_z[:, None] + step_z[None]) % N_GZ
    export_global = ghost_export.reshape(device_count, exported) + (devices * per_device)[:, None]
    ghost_global = export_global[partner_device]
    lookup = jnp.concatenate([devices[:, None] * per_device + jnp.arange(per_device, dtype=jnp.int32)[None, :], ghost_global.reshape(device_count, 27 * exported)], axis=1).astype(jnp.int32)
    slot_shift = jnp.stack([step_x * CX, step_y * CY, step_z * CZ]).astype(jnp.float32)
    shift_table = jnp.concatenate([jnp.zeros((3, per_device), jnp.float32), jnp.repeat(slot_shift, exported, axis=1)], axis=1)
    cell_float = atom_cell.astype(jnp.float32)
    up_all = jnp.dot(w_up, features, preferred_element_type=jnp.float32).astype(jnp.bfloat16)
    charges = jnp.dot(charge_weight, features, preferred_element_type=jnp.float32)

    def short_energy(fraction):
        positions = cell_float + fraction

        def device_energy(device):
            row_ids = lookup[device]
            pos_table = jnp.take(positions, row_ids, axis=1) + shift_table
            up_table = jnp.take(up_all, row_ids, axis=1)

            def one_block(number):
                first_row = (device * per_device + number * BLOCK).astype(jnp.int32)
                return block_energy(pos_table, up_table, lax.dynamic_slice_in_dim(positions, first_row, BLOCK, 1), lax.dynamic_slice_in_dim(features, first_row, BLOCK, 1), lax.dynamic_slice_in_dim(neighbors, first_row, BLOCK, 0), lax.dynamic_slice_in_dim(neighbor_count, first_row, BLOCK, 0), radial_weight, w_out, energy_weight)
            return lax.map(one_block, jnp.arange(per_device // BLOCK, dtype=jnp.int32)).reshape(-1)
        return lax.map(jax.checkpoint(device_energy), devices).reshape(-1)
    anchor_x = jnp.repeat(coord_x * CX, per_device)
    anchor_y = jnp.repeat(coord_y * CY, per_device)
    anchor_z = jnp.repeat(coord_z * CZ, per_device)
    node_x = atom_cell[0] + anchor_x - 1
    node_y = atom_cell[1] + anchor_y - 1
    node_z = atom_cell[2] + anchor_z - 1
    influence = influence_of(wave_number(jnp.arange(GX), GX), wave_number(jnp.arange(GY), GY), wave_number(jnp.arange(GZ), GZ), GX * GY * GZ)

    def long_energy(fraction, charge_values):
        weights = spline_weights(fraction)
        density = jnp.zeros((GX, GY, GZ), jnp.float32)
        for step_one in range(4):
            for step_two in range(4):
                for step_three in range(4):
                    amount = charge_values * weights[step_one][0] * weights[step_two][1] * weights[step_three][2]
                    density = density.at[(node_x + step_one) % GX, (node_y + step_two) % GY, (node_z + step_three) % GZ].add(amount)
        spectrum = jnp.fft.fftn(density)
        power = spectrum.real ** 2 + spectrum.imag ** 2
        return 0.5 * jnp.sum(influence * power)

    def total_energy(fraction, charge_values):
        atom_short = short_energy(fraction)
        return (jnp.sum(atom_short) + long_energy(fraction, charge_values), atom_short)
    (energy_total, atom_short), (grad_frac, grad_charge) = jax.value_and_grad(total_energy, argnums=(0, 1), has_aux=True)(atom_frac.astype(jnp.float32), charges)
    forces = -grad_frac
    atom_energy = atom_short + 0.5 * charges * grad_charge
    return (forces, atom_energy)
```

```python
import math

import jax
import jax.numpy as jnp
import numpy as np
from jax import lax
from jax.experimental import pallas as pl
from jax.experimental.pallas import tpu as pltpu
from jax.sharding import PartitionSpec as P

CX, CY, CZ = 8, 16, 64
HALO_X, HALO_Y, HALO_Z = CX + 3, CY + 3, CZ + 3
PER_HALF = 128 // HALO_Y
NX, NY, NZ = 16, 4, 4
PLANES = NX * NY
NEIGHBORS = 32
EXPORTED = 64
ATOMS = 256
CHANNELS = 128
ROWS = CHANNELS + 16
BLOCKS = 8

basis_step = 1.4
basis_width = 1.4
message_scale = 0.125
vector_scale = 1.0 / 6.0
ewald_beta_sq = 2.0

F32 = jnp.float32
BF16 = jnp.bfloat16
MESH = pl.DeviceIdType.MESH
HIGHEST = lax.Precision.HIGHEST

SLOTS = [(s, s // 9 - 1, s // 3 % 3 - 1, s % 3 - 1) for s in range(27)]
LENT = [slot for slot in SLOTS if slot[0] != 13]
WINDOWS = [(x, x // PER_HALF, HALO_Y * (x % PER_HALF)) for x in range(HALO_X)]


def trig_basis(extent):
    cells = np.arange(extent)
    half = extent // 2
    rows, numbers = [], []
    for k in range(half + 1):
        scale = math.sqrt((1.0 if k in (0, half) else 2.0) / extent)
        rows.append(scale * np.cos(2.0 * math.pi * (k * cells % extent) / extent))
        numbers.append(k)
    for k in range(1, half):
        rows.append(math.sqrt(2.0 / extent) * np.sin(2.0 * math.pi * (k * cells % extent) / extent))
        numbers.append(k)
    return np.array(rows), np.array(numbers)


def tables():
    wave_x, number_x = trig_basis(CX * NX)
    wave_y, number_y = trig_basis(CY * NY)
    wave_z, _ = trig_basis(CZ * NZ)
    along_z = np.zeros((NZ, CZ * NZ, 128), np.float32)
    for l in range(NZ):
        along_z[l, :, :HALO_Z] = wave_z[:, (l * CZ - 1 + np.arange(HALO_Z)) % (CZ * NZ)]
    along_x = np.zeros((CX * NX, 256), np.float32)
    for x in range(HALO_X):
        for i in range(NX):
            along_x[:, x * NX + i] = wave_x[:, (i * CX + x - 1) % (CX * NX)]
    along_y = np.zeros((128, 128), np.float32)
    for j in range(NY):
        for y in range(HALO_Y):
            along_y[: CY * NY, 32 * j + y] = wave_y[:, (j * CY + y - 1) % (CY * NY)]
    square = np.zeros((128, 128), np.float32)
    square[:, : CY * NY] = (2.0 * math.pi / (CX * NX) * number_x[:, None]) ** 2 + (
        2.0 * math.pi / (CY * NY) * number_y[None, :]
    ) ** 2
    square[:, CY * NY :] = 1.0
    return along_z, along_x, along_x.T.copy(), along_y, along_y.T.copy(), square


def spline_weights(t):
    r = 1.0 - t
    t2 = t * t
    t3 = t2 * t
    values = (
        r * r * r / 6.0,
        (3.0 * t3 - 6.0 * t2 + 4.0) / 6.0,
        (-3.0 * t3 + 3.0 * t2 + 3.0 * t + 1.0) / 6.0,
        t3 / 6.0,
    )
    slopes = (-0.5 * r * r, 1.5 * t2 - 2.0 * t, -1.5 * t2 + t + 0.5, 0.5 * t2)
    return values, slopes


def node_rows(count, cell, parts):
    gap = lax.broadcasted_iota(jnp.int32, (count, ATOMS), 0) - cell
    total = jnp.zeros((count, ATOMS), F32)
    for s in range(4):
        total = jnp.where(gap == s, parts[s], total)
    return total


def dot(a, b, precision=None):
    return jnp.dot(a, b, precision=precision, preferred_element_type=F32)


def dot_nt(a, b, precision=None):
    return lax.dot_general(
        a, b, (((1,), (1,)), ((), ())), precision=precision, preferred_element_type=F32
    )


def halves(x):
    high = x.astype(BF16).astype(F32)
    return high, x - high


def kernel(
    cell_ref,
    frac_ref,
    feat_ref,
    export_ref,
    neighbor_ref,
    count_ref,
    w_up_ref,
    radial_ref,
    w_out_ref,
    energy_ref,
    charge_ref,
    along_z_ref,
    along_x_ref,
    along_xt_ref,
    along_y_ref,
    along_yt_ref,
    square_ref,
    forces_ref,
    atom_energy_ref,
    parts_out,
    parts_in,
    planes_out,
    planes_in,
    back_out,
    back_in,
    modes,
    lend_out,
    ghosts,
    grads_out,
    grads_in,
    place,
    z_waves,
    z_slopes,
    window,
    table,
    gathered,
    radials,
    messages,
    turned,
    hots,
    lows,
    highs,
    relatives,
    inverses,
    sums,
    pushed,
    parts_send,
    parts_recv,
    planes_send,
    planes_recv,
    back_send,
    back_recv,
    modes_send,
    modes_recv,
    lend_send,
    lend_recv,
    grads_send,
    grads_recv,
):
    gx, gy, gz = lax.axis_index("gx"), lax.axis_index("gy"), lax.axis_index("gz")
    me = gy * NX + gx

    def shifted(a, b, c):
        return (lax.rem(gx + a + NX, NX), lax.rem(gy + b + NY, NY), lax.rem(gz + c + NZ, NZ))

    def over_planes(action):
        for dy in range(NY):

            def step(dx, carry):
                x, y = lax.rem(gx + dx, NX), lax.rem(gy + dy, NY)
                action(x, y, y * NX + x)
                return carry

            lax.fori_loop(1 if dy == 0 else 0, NX, step, 0)

    barrier = pltpu.get_barrier_semaphore()

    def greet(device):
        pl.semaphore_signal(barrier, inc=1, device_id=device, device_id_type=MESH)

    for c in range(1, NZ):
        greet((gx, gy, lax.rem(gz + c, NZ)))
    over_planes(lambda x, y, p: greet((x, y, gz)))
    for s, a, b, c in LENT:
        greet(shifted(-a, -b, -c))

    feat = feat_ref[...]
    cell = cell_ref[...]
    frac = frac_ref[...].astype(F32)
    up = dot(w_up_ref[...], feat).astype(BF16)
    charge = dot(jnp.broadcast_to(charge_ref[...], (16, CHANNELS)), feat)[0:1, :]
    place[...] = jnp.zeros_like(place)
    place[0:3, :] = cell.astype(F32)
    place[8:11, :] = frac
    spot = place[...]
    export = export_ref[...]
    pick_t = (lax.broadcasted_iota(jnp.int32, (ATOMS, 128), 0) == export).astype(F32)
    pick = pick_t.T
    lend_out[0:EXPORTED, :] = dot_nt(pick[0:EXPORTED].astype(BF16), up).astype(BF16)
    lend_out[EXPORTED : EXPORTED + 16, :] = dot(spot.astype(BF16), pick_t.astype(BF16)).astype(BF16)

    values, slopes = spline_weights(frac)
    along_z = along_z_ref[gz]
    z_waves[...] = dot(
        along_z, node_rows(128, cell[2:3], [v[2:3] for v in values]), HIGHEST
    )
    rows_x = node_rows(16, cell[0:1], [v[0:1] for v in values])
    rows_y = node_rows(24, cell[1:2], [v[1:2] for v in values])
    window[...] = jnp.zeros_like(window)
    for x, half, lane in WINDOWS:
        at = pl.ds(128 * half + lane, HALO_Y)
        window[at, 0:ATOMS] = rows_x[x : x + 1] * rows_y[0:HALO_Y]
    waves = dot_nt(z_waves[...] * charge, window[:, 0:ATOMS], HIGHEST)
    for l in range(NZ):
        parts_out[l] = waves[PLANES * l : PLANES * (l + 1)]

    pl.semaphore_wait(barrier, (NZ - 1) + (PLANES - 1) + len(LENT))

    def part_copy(c):
        l = lax.rem(gz + c, NZ)
        return pltpu.make_async_remote_copy(
            src_ref=parts_out.at[l],
            dst_ref=parts_in.at[gz],
            send_sem=parts_send.at[c],
            recv_sem=parts_recv.at[NZ - c],
            device_id=(gx, gy, l),
            device_id_type=MESH,
        )

    def part_arrival(c):
        l = lax.rem(gz + c, NZ)
        return pltpu.make_async_remote_copy(
            src_ref=parts_out.at[l],
            dst_ref=parts_in.at[l],
            send_sem=parts_send.at[c],
            recv_sem=parts_recv.at[c],
            device_id=(gx, gy, l),
            device_id_type=MESH,
        )

    def lend_copy(s, a, b, c):
        return pltpu.make_async_remote_copy(
            src_ref=lend_out,
            dst_ref=ghosts.at[s],
            send_sem=lend_send.at[s],
            recv_sem=lend_recv.at[s],
            device_id=shifted(-a, -b, -c),
            device_id_type=MESH,
        )

    for c in range(1, NZ):
        part_copy(c).start()
    for slot in LENT:
        lend_copy(*slot).start()

    z_slopes[...] = dot(
        along_z, node_rows(128, cell[2:3], [v[2:3] for v in slopes]), HIGHEST
    )
    slope_x = node_rows(16, cell[0:1], [v[0:1] for v in slopes])
    slope_y = node_rows(24, cell[1:2], [v[1:2] for v in slopes])
    for x, half, lane in WINDOWS:
        at = pl.ds(128 * half + lane, HALO_Y)
        window[at, ATOMS : 2 * ATOMS] = slope_x[x : x + 1] * rows_y[0:HALO_Y]
        window[at, 2 * ATOMS : 3 * ATOMS] = rows_x[x : x + 1] * slope_y[0:HALO_Y]
    parts_in[gz] = parts_out[gz]
    ghosts[13] = jnp.zeros((EXPORTED + 16, 128), BF16)
    ghosts[27] = jnp.zeros((EXPORTED + 16, 128), BF16)
    table[0:CHANNELS, :] = up
    table[CHANNELS:ROWS, :] = spot.astype(BF16)

    for c in range(1, NZ):
        part_arrival(c).wait_recv()
    total = parts_in[0] + parts_in[1] + parts_in[2] + parts_in[3]
    planes_out[:, 0, :] = total[:, 0:128]
    planes_out[:, 1, :] = total[:, 128:256]

    def plane_copy(x, y, p):
        return pltpu.make_async_remote_copy(
            src_ref=planes_out.at[p],
            dst_ref=planes_in.at[me],
            send_sem=planes_send,
            recv_sem=planes_recv,
            device_id=(x, y, gz),
            device_id_type=MESH,
        )

    over_planes(lambda x, y, p: plane_copy(x, y, p).start())
    planes_in[me] = planes_out[me]

    for slot in LENT:
        lend_copy(*slot).wait_recv()
    row = lax.broadcasted_iota(jnp.int32, (16, 128), 0)
    lane = lax.broadcasted_iota(jnp.int32, (16, 128), 1)
    for h in range(1, BLOCKS):
        first = 4 * (h - 1)
        lent = jnp.concatenate([ghosts[first + q, 0:EXPORTED, :] for q in range(4)], axis=0)
        table[ROWS * h : ROWS * h + CHANNELS, :] = lent.astype(F32).T.astype(BF16)
        spots = []
        for q in range(4):
            s = first + q
            a, b, c = (s // 9 - 1, s // 3 % 3 - 1, s % 3 - 1)
            far = jnp.where(
                row == 0,
                float(a * CX),
                jnp.where(row == 1, float(b * CY), jnp.where(row == 2, float(c * CZ), 0.0)),
            )
            spots.append(ghosts[s, EXPORTED : EXPORTED + 16, :].astype(F32) + far)
        at = slice(ROWS * h + CHANNELS, ROWS * (h + 1))
        table[at, 0:128] = jnp.where(lane < EXPORTED, spots[0], spots[1]).astype(BF16)
        table[at, 128:256] = jnp.where(lane < EXPORTED, spots[2], spots[3]).astype(BF16)

    entry = neighbor_ref[...]
    eye = (
        lax.broadcasted_iota(jnp.int32, (NEIGHBORS, NEIGHBORS), 0)
        == lax.broadcasted_iota(jnp.int32, (NEIGHBORS, NEIGHBORS), 1)
    ).astype(BF16)
    lows[...] = dot_nt(eye, (entry & 255).astype(F32).astype(BF16)).astype(jnp.int32)
    highs[...] = dot_nt(eye, (entry >> 8).astype(F32).astype(BF16)).astype(jnp.int32)

    weight_high, weight_low = halves(radial_ref[...])
    stack = lax.broadcasted_iota(jnp.int32, (8, 24), 1)
    basis_row = lax.broadcasted_iota(jnp.int32, (8, 24), 0)
    hit = lax.rem(stack, 8) == basis_row
    to_high = jnp.logical_and(hit, stack < 16).astype(BF16)
    to_low = jnp.logical_and(hit, stack >= 16).astype(BF16)
    weights = (
        dot(weight_high.astype(BF16), to_high) + dot(weight_low.astype(BF16), to_low)
    ).astype(BF16)

    here = spot[0:8] + spot[8:16]
    count = count_ref[...]
    for a in range(4):
        sums[a] = jnp.zeros((CHANNELS, ATOMS), F32)
    sub = lax.broadcasted_iota(jnp.int32, (ATOMS, 2 * ATOMS), 0)
    centre = lax.broadcasted_iota(jnp.int32, (8, 2 * ATOMS), 0).astype(F32) * basis_step

    def gather(pair, carry):
        k = 2 * pair
        low = jnp.concatenate([lows[pl.ds(k, 1), :], lows[pl.ds(k + 1, 1), :]], axis=1)
        high = jnp.concatenate([highs[pl.ds(k, 1), :], highs[pl.ds(k + 1, 1), :]], axis=1)
        hot = jnp.where(sub == low, 1.0, 0.0).astype(BF16)
        hots[pair] = hot
        gathered[...] = dot(table[...], hot)
        high8 = jnp.broadcast_to(high, (8, 2 * ATOMS))

        def chosen(start):
            result = gathered[pl.ds(start, 8), :]
            for h in range(1, BLOCKS):
                result = jnp.where(high8 == h, gathered[pl.ds(start + ROWS * h, 8), :], result)
            return result

        there = chosen(CHANNELS) + chosen(CHANNELS + 8)
        rel = there - jnp.concatenate([here, here], axis=1)
        dist = jnp.sqrt(jnp.sum(rel * rel, axis=0, keepdims=True) + 1.0)
        used = jnp.concatenate([count > k, count > k + 1], axis=1).astype(F32)
        gap = (dist - centre) / basis_width
        basis = jnp.exp(-(gap * gap)) * used
        slope = basis * gap * (-2.0 / basis_width)
        basis_high, basis_low = halves(basis)
        slope_high, slope_low = halves(slope)
        radials[0:CHANNELS, :] = dot(
            weights, jnp.concatenate([basis_high, basis_low, basis_high], axis=0).astype(BF16)
        )
        radials[CHANNELS : 2 * CHANNELS, :] = dot(
            weights, jnp.concatenate([slope_high, slope_low, slope_high], axis=0).astype(BF16)
        )
        inverse = 1.0 / dist
        relatives[k] = rel[:, 0:ATOMS]
        relatives[k + 1] = rel[:, ATOMS:]
        inverses[k] = jnp.broadcast_to(inverse[:, 0:ATOMS], (8, ATOMS))
        inverses[k + 1] = jnp.broadcast_to(inverse[:, ATOMS:], (8, ATOMS))
        along = [jnp.broadcast_to(rel[a : a + 1], (8, 2 * ATOMS)) for a in range(3)]
        for c in range(0, CHANNELS, 8):
            at = pl.ds(c, 8)
            source = chosen(c)
            message = radials[at, :] * source
            turn = radials[pl.ds(CHANNELS + c, 8), :] * source
            messages[k, at, :] = message[:, 0:ATOMS]
            messages[k + 1, at, :] = message[:, ATOMS:]
            turned[k, at, :] = turn[:, 0:ATOMS]
            turned[k + 1, at, :] = turn[:, ATOMS:]
            sums[0, at, :] += message[:, 0:ATOMS] + message[:, ATOMS:]
            for a in range(3):
                moved = message * along[a]
                sums[a + 1, at, :] += moved[:, 0:ATOMS] + moved[:, ATOMS:]
        return carry

    lax.fori_loop(0, NEIGHBORS // 2, gather, 0)

    scalar = sums[0] * message_scale
    vector = [sums[a + 1] * (message_scale * vector_scale) for a in range(3)]
    invariant = scalar + scalar * scalar + (
        vector[0] * vector[0] + vector[1] * vector[1] + vector[2] * vector[2]
    )
    w_out = w_out_ref[...]
    hidden = feat.astype(F32) + dot(w_out, invariant.astype(BF16))
    wide = (
        lax.broadcasted_iota(jnp.int32, (CHANNELS, CHANNELS), 0)
        == lax.broadcasted_iota(jnp.int32, (CHANNELS, CHANNELS), 1)
    ).astype(BF16)
    readout = dot_nt(wide, jnp.broadcast_to(energy_ref[...], (16, CHANNELS)))[:, 0:1]
    gate = 1.0 / (1.0 + jnp.exp(-hidden))
    short = jnp.sum(readout * (hidden * gate), axis=0, keepdims=True)
    d_hidden = readout * (gate * (1.0 + hidden * (1.0 - gate)))
    back_high, back_low = halves(d_hidden)
    w_out_t = w_out.astype(F32).T.astype(BF16)
    d_invariant = dot(w_out_t, back_high.astype(BF16)) + dot(w_out_t, back_low.astype(BF16))
    d_invariant = d_invariant.astype(BF16).astype(F32)
    sums[0] = d_invariant * (1.0 + 2.0 * scalar) * message_scale
    for a in range(3):
        sums[a + 1] = d_invariant * vector[a] * (2.0 * message_scale * vector_scale)

    pltpu.make_async_remote_copy(
        src_ref=planes_out.at[pl.ds(0, PLANES - 1)],
        dst_ref=planes_in.at[pl.ds(0, PLANES - 1)],
        send_sem=planes_send,
        recv_sem=planes_recv,
        device_id=(gx, gy, gz),
        device_id_type=MESH,
    ).wait_recv()
    plane = [planes_in[:, 0, :], planes_in[:, 1, :]]
    spread = []
    for x, half, at in WINDOWS:
        line = jnp.zeros((NX, 128), F32)
        for j in range(NY):
            piece = plane[half][NX * j : NX * (j + 1)]
            piece = pltpu.roll(piece, (32 * j - at) % 128, 1)
            inside = jnp.logical_and(lane >= 32 * j, lane < 32 * j + HALO_Y)
            line = jnp.where(inside, piece, line)
        spread.append(line)
    spread.append(jnp.zeros((256 - NX * HALO_X, 128), F32))
    lines = jnp.concatenate(spread, axis=0)
    spectrum = dot(along_x_ref[...], dot(lines, along_yt_ref[...], HIGHEST), HIGHEST)
    mode = gz * PLANES + me
    number = jnp.where(mode <= CZ * NZ // 2, mode, mode - CZ * NZ // 2).astype(F32)
    wave = number * (2.0 * math.pi / (CZ * NZ))
    square = square_ref[...] + wave * wave
    positive = square > 0.0
    safe = jnp.where(positive, square, 1.0)
    filtered = spectrum * jnp.where(
        positive, 4.0 * math.pi * jnp.exp(-square / (4.0 * ewald_beta_sq)) / safe, 0.0
    )
    lines = dot(dot(along_xt_ref[...], filtered, HIGHEST), along_y_ref[...], HIGHEST)
    for j in range(NY):
        for half in range(2):
            piece = jnp.zeros((NX, 128), F32)
            for x, which, at in WINDOWS:
                if which == half:
                    line = pltpu.roll(lines[NX * x : NX * (x + 1)], (at - 32 * j) % 128, 1)
                    inside = jnp.logical_and(lane >= at, lane < at + HALO_Y)
                    piece = jnp.where(inside, line, piece)
            back_out[NX * j : NX * (j + 1), half, :] = piece

    def back_copy(x, y, p):
        return pltpu.make_async_remote_copy(
            src_ref=back_out.at[p],
            dst_ref=back_in.at[me],
            send_sem=back_send,
            recv_sem=back_recv,
            device_id=(x, y, gz),
            device_id_type=MESH,
        )

    over_planes(lambda x, y, p: back_copy(x, y, p).start())
    back_in[me] = back_out[me]

    pushed[...] = jnp.zeros_like(pushed)

    def derive(pair, total):
        k = 2 * pair
        pushes = []
        for e in range(2):
            rel = relatives[k + e]
            along = [jnp.broadcast_to(rel[a : a + 1], (8, ATOMS)) for a in range(3)]
            stretch = jnp.zeros((8, ATOMS), F32)
            direct = [jnp.zeros((8, ATOMS), F32) for _ in range(3)]
            for c in range(0, CHANNELS, 8):
                at = pl.ds(c, 8)
                message = messages[k + e, at, :]
                d_message = sums[0, at, :]
                for a in range(3):
                    d_vector = sums[a + 1, at, :]
                    d_message += d_vector * along[a]
                    direct[a] += d_vector * message
                stretch += d_message * turned[k + e, at, :]
            pull = jnp.sum(stretch, axis=0, keepdims=True) * inverses[k + e][0:1]
            rows = [jnp.sum(direct[a], axis=0, keepdims=True) + pull * rel[a : a + 1] for a in range(3)]
            push = jnp.concatenate(rows + [jnp.zeros((5, ATOMS), F32)], axis=0)
            total = total + push
            pushes.append(push)
        push = jnp.concatenate(pushes, axis=1)
        high = jnp.concatenate([highs[pl.ds(k, 1), :], highs[pl.ds(k + 1, 1), :]], axis=1)
        push_high, push_low = halves(push)
        masks = [high == h for h in range(BLOCKS)]
        left = jnp.concatenate(
            [jnp.where(mask, push_high, 0.0) for mask in masks]
            + [jnp.where(mask, push_low, 0.0) for mask in masks],
            axis=0,
        ).astype(BF16)
        pushed[...] += dot_nt(left, hots[pair])
        return total

    pulled = lax.fori_loop(0, NEIGHBORS // 2, derive, jnp.zeros((8, ATOMS), F32))
    reach = pushed[0 : 8 * BLOCKS, :] + pushed[8 * BLOCKS : 16 * BLOCKS, :]
    for s, a, b, c in LENT:
        h, q = s // 4 + 1, s % 4
        piece = reach[8 * h : 8 * (h + 1), 128 * (q // 2) : 128 * (q // 2 + 1)]
        grads_out[s] = pltpu.roll(piece, 64, 1) if q % 2 else piece

    def grads_copy(s, a, b, c):
        return pltpu.make_async_remote_copy(
            src_ref=grads_out.at[s],
            dst_ref=grads_in.at[s],
            send_sem=grads_send.at[s],
            recv_sem=grads_recv.at[s],
            device_id=shifted(a, b, c),
            device_id_type=MESH,
        )

    for slot in LENT:
        grads_copy(*slot).start()

    pltpu.make_async_remote_copy(
        src_ref=back_out.at[pl.ds(0, PLANES - 1)],
        dst_ref=back_in.at[pl.ds(0, PLANES - 1)],
        send_sem=back_send,
        recv_sem=back_recv,
        device_id=(gx, gy, gz),
        device_id_type=MESH,
    ).wait_recv()
    modes[gz, :, 0:128] = back_in[:, 0, :]
    modes[gz, :, 128:256] = back_in[:, 1, :]

    def mode_copy(c):
        return pltpu.make_async_remote_copy(
            src_ref=modes.at[gz],
            dst_ref=modes.at[gz],
            send_sem=modes_send.at[c],
            recv_sem=modes_recv.at[NZ - c],
            device_id=(gx, gy, lax.rem(gz + c, NZ)),
            device_id_type=MESH,
        )

    def mode_arrival(c):
        l = lax.rem(gz + c, NZ)
        return pltpu.make_async_remote_copy(
            src_ref=modes.at[gz],
            dst_ref=modes.at[l],
            send_sem=modes_send.at[c],
            recv_sem=modes_recv.at[c],
            device_id=(gx, gy, l),
            device_id_type=MESH,
        )

    for c in range(1, NZ):
        mode_copy(c).start()

    for slot in LENT:
        grads_copy(*slot).wait_recv()
    returned = grads_in[LENT[0][0]]
    for slot in LENT[1:]:
        returned = returned + grads_in[slot[0]]
    keep = jnp.where(lax.broadcasted_iota(jnp.int32, (128, ATOMS), 0) < EXPORTED, pick, 0.0)
    grad = reach[0:8] - pulled + dot(returned, keep, HIGHEST)

    for c in range(1, NZ):
        mode_arrival(c).wait_recv()
    field = dot(
        jnp.concatenate([modes[l] for l in range(NZ)], axis=0), window[...], HIGHEST
    )
    here_waves = z_waves[...]
    potential = jnp.sum(here_waves * field[:, 0:ATOMS], axis=0, keepdims=True)
    along_first = jnp.sum(here_waves * field[:, ATOMS : 2 * ATOMS], axis=0, keepdims=True)
    along_second = jnp.sum(here_waves * field[:, 2 * ATOMS :], axis=0, keepdims=True)
    along_third = jnp.sum(z_slopes[...] * field[:, 0:ATOMS], axis=0, keepdims=True)
    forces_ref[0:1, :] = -(grad[0:1] + charge * along_first)
    forces_ref[1:2, :] = -(grad[1:2] + charge * along_second)
    forces_ref[2:3, :] = -(grad[2:3] + charge * along_third)
    atom_energy_ref[...] = short + 0.5 * charge * potential

    for c in range(1, NZ):
        part_copy(c).wait_send()
        mode_copy(c).wait_send()
    for slot in LENT:
        lend_copy(*slot).wait_send()
        grads_copy(*slot).wait_send()
    pltpu.make_async_remote_copy(
        src_ref=planes_out.at[pl.ds(0, PLANES - 1)],
        dst_ref=planes_in.at[pl.ds(0, PLANES - 1)],
        send_sem=planes_send,
        recv_sem=planes_recv,
        device_id=(gx, gy, gz),
        device_id_type=MESH,
    ).wait_send()
    pltpu.make_async_remote_copy(
        src_ref=back_out.at[pl.ds(0, PLANES - 1)],
        dst_ref=back_in.at[pl.ds(0, PLANES - 1)],
        send_sem=back_send,
        recv_sem=back_recv,
        device_id=(gx, gy, gz),
        device_id_type=MESH,
    ).wait_send()


def per_device(
    atom_cell,
    atom_frac,
    features,
    ghost_export,
    neighbors,
    neighbor_count,
    w_up,
    radial_weight,
    w_out,
    energy_weight,
    charge_weight,
):
    vmem = pl.BlockSpec(memory_space=pltpu.VMEM)
    constants = tables()
    dma = pltpu.SemaphoreType.DMA
    forces, atom_energy = pl.pallas_call(
        kernel,
        name="layer",
        out_shape=(
            jax.ShapeDtypeStruct((3, ATOMS), F32),
            jax.ShapeDtypeStruct((1, ATOMS), F32),
        ),
        in_specs=[vmem] * (11 + len(constants)),
        out_specs=(vmem, vmem),
        scratch_shapes=[
            pltpu.VMEM((NZ, PLANES, 256), F32),
            pltpu.VMEM((NZ, PLANES, 256), F32),
            pltpu.VMEM((PLANES, 2, 128), F32),
            pltpu.VMEM((PLANES, 2, 128), F32),
            pltpu.VMEM((PLANES, 2, 128), F32),
            pltpu.VMEM((PLANES, 2, 128), F32),
            pltpu.VMEM((NZ, PLANES, 256), F32),
            pltpu.VMEM((EXPORTED + 16, 128), BF16),
            pltpu.VMEM((28, EXPORTED + 16, 128), BF16),
            pltpu.VMEM((27, 8, 128), F32),
            pltpu.VMEM((27, 8, 128), F32),
            pltpu.VMEM((16, ATOMS), F32),
            pltpu.VMEM((CZ * NZ, ATOMS), F32),
            pltpu.VMEM((CZ * NZ, ATOMS), F32),
            pltpu.VMEM((256, 3 * ATOMS), F32),
            pltpu.VMEM((BLOCKS * ROWS, 256), BF16),
            pltpu.VMEM((BLOCKS * ROWS, 2 * ATOMS), F32),
            pltpu.VMEM((2 * CHANNELS, 2 * ATOMS), F32),
            pltpu.VMEM((NEIGHBORS, CHANNELS, ATOMS), F32),
            pltpu.VMEM((NEIGHBORS, CHANNELS, ATOMS), F32),
            pltpu.VMEM((NEIGHBORS // 2, 256, 2 * ATOMS), BF16),
            pltpu.VMEM((NEIGHBORS, ATOMS), jnp.int32),
            pltpu.VMEM((NEIGHBORS, ATOMS), jnp.int32),
            pltpu.VMEM((NEIGHBORS, 8, ATOMS), F32),
            pltpu.VMEM((NEIGHBORS, 8, ATOMS), F32),
            pltpu.VMEM((4, CHANNELS, ATOMS), F32),
            pltpu.VMEM((16 * BLOCKS, 256), F32),
            dma((NZ,)),
            dma((NZ,)),
            dma,
            dma,
            dma,
            dma,
            dma((NZ,)),
            dma((NZ,)),
            dma((27,)),
            dma((27,)),
            dma((27,)),
            dma((27,)),
        ],
        compiler_params=pltpu.CompilerParams(collective_id=0, has_side_effects=True),
    )(
        atom_cell,
        atom_frac,
        features,
        jnp.concatenate([ghost_export, ghost_export]).reshape(1, 2 * EXPORTED),
        neighbors,
        neighbor_count.reshape(1, ATOMS),
        w_up,
        radial_weight,
        w_out,
        energy_weight.reshape(1, CHANNELS),
        charge_weight.reshape(1, CHANNELS),
        *constants,
    )
    return forces, atom_energy.reshape(ATOMS)


def solution(mesh):
    whole = ("gx", "gy", "gz")
    in_specs = (
        P(None, whole),
        P(None, whole),
        P(None, whole),
        P(whole),
        P(whole, None),
        P(whole),
        P(),
        P(),
        P(),
        P(),
        P(),
    )
    out_specs = (P(None, whole), P(whole))
    return jax.shard_map(
        per_device, mesh=mesh, in_specs=in_specs, out_specs=out_specs, check_vma=False
    )
```

```python
import math

import jax
import jax.numpy as jnp
import numpy as np
from jax import lax
from jax.experimental import pallas as pl
from jax.experimental.pallas import tpu as pltpu
from jax.sharding import PartitionSpec as P

CX, CY, CZ = 8, 16, 64
HALO_X, HALO_Y, HALO_Z = CX + 3, CY + 3, CZ + 3
PER_HALF = 128 // HALO_Y
NX, NY, NZ = 16, 4, 4
PLANES = NX * NY
NEIGHBORS = 32
EXPORTED = 64
ATOMS = 256
CHANNELS = 128
ROWS = CHANNELS + 16
BLOCKS = 8

basis_step = 1.4
basis_width = 1.4
message_scale = 0.125
vector_scale = 1.0 / 6.0
ewald_beta_sq = 2.0

F32 = jnp.float32
BF16 = jnp.bfloat16
MESH = pl.DeviceIdType.MESH
HIGHEST = lax.Precision.HIGHEST

SLOTS = [(s, s // 9 - 1, s // 3 % 3 - 1, s % 3 - 1) for s in range(27)]
LENT = [slot for slot in SLOTS if slot[0] != 13]
BESIDE = [(b, c) for _, a, b, c in LENT if a == 0]
WINDOWS = [(x, x // PER_HALF, HALO_Y * (x % PER_HALF)) for x in range(HALO_X)]


def trig_basis(extent):
    cells = np.arange(extent)
    half = extent // 2
    rows, numbers = [], []
    for k in range(half + 1):
        scale = math.sqrt((1.0 if k in (0, half) else 2.0) / extent)
        rows.append(scale * np.cos(2.0 * math.pi * (k * cells % extent) / extent))
        numbers.append(k)
    for k in range(1, half):
        rows.append(math.sqrt(2.0 / extent) * np.sin(2.0 * math.pi * (k * cells % extent) / extent))
        numbers.append(k)
    return np.array(rows), np.array(numbers)


def tables():
    wave_x, number_x = trig_basis(CX * NX)
    wave_y, number_y = trig_basis(CY * NY)
    wave_z, _ = trig_basis(CZ * NZ)
    along_z = np.zeros((NZ, CZ * NZ, 128), np.float32)
    for l in range(NZ):
        along_z[l, :, :HALO_Z] = wave_z[:, (l * CZ - 1 + np.arange(HALO_Z)) % (CZ * NZ)]
    along_x = np.zeros((CX * NX, 256), np.float32)
    for x in range(HALO_X):
        for i in range(NX):
            along_x[:, x * NX + i] = wave_x[:, (i * CX + x - 1) % (CX * NX)]
    along_y = np.zeros((128, 128), np.float32)
    for j in range(NY):
        for y in range(HALO_Y):
            along_y[: CY * NY, 32 * j + y] = wave_y[:, (j * CY + y - 1) % (CY * NY)]
    square = np.zeros((128, 128), np.float32)
    square[:, : CY * NY] = (2.0 * math.pi / (CX * NX) * number_x[:, None]) ** 2 + (
        2.0 * math.pi / (CY * NY) * number_y[None, :]
    ) ** 2
    square[:, CY * NY :] = 1.0
    return along_z, along_x, along_x.T.copy(), along_y, along_y.T.copy(), square


def spline_weights(t):
    r = 1.0 - t
    t2 = t * t
    t3 = t2 * t
    values = (
        r * r * r / 6.0,
        (3.0 * t3 - 6.0 * t2 + 4.0) / 6.0,
        (-3.0 * t3 + 3.0 * t2 + 3.0 * t + 1.0) / 6.0,
        t3 / 6.0,
    )
    slopes = (-0.5 * r * r, 1.5 * t2 - 2.0 * t, -1.5 * t2 + t + 0.5, 0.5 * t2)
    return values, slopes


def node_rows(count, cell, parts):
    gap = lax.broadcasted_iota(jnp.int32, (count, ATOMS), 0) - cell
    total = jnp.zeros((count, ATOMS), F32)
    for s in range(4):
        total = jnp.where(gap == s, parts[s], total)
    return total


def dot(a, b, precision=None):
    return jnp.dot(a, b, precision=precision, preferred_element_type=F32)


def dot_nt(a, b, precision=None):
    return lax.dot_general(
        a, b, (((1,), (1,)), ((), ())), precision=precision, preferred_element_type=F32
    )


def halves(x):
    high = x.astype(BF16).astype(F32)
    return high, x - high


def kernel(
    cell_ref,
    frac_ref,
    feat_ref,
    export_ref,
    neighbor_ref,
    count_ref,
    w_up_ref,
    radial_ref,
    w_out_ref,
    energy_ref,
    charge_ref,
    along_z_ref,
    along_x_ref,
    along_xt_ref,
    along_y_ref,
    along_yt_ref,
    square_ref,
    forces_ref,
    atom_energy_ref,
    parts_out,
    parts_in,
    planes_out,
    planes_in,
    back_out,
    back_in,
    modes,
    ghosts,
    grads_out,
    grads_in,
    place,
    z_waves,
    z_slopes,
    window,
    table,
    gathered,
    partial,
    radials,
    messages,
    turned,
    hots,
    lows,
    highs,
    relatives,
    inverses,
    sums,
    pushed,
    parts_send,
    parts_recv,
    planes_send,
    planes_recv,
    back_send,
    back_recv,
    modes_send,
    modes_recv,
    beside_send,
    beside_recv,
    far_send,
    far_recv,
    beyond_send,
    beyond_recv,
    near_send,
    near_recv,
    grads_send,
    grads_recv,
):
    gx, gy, gz = lax.axis_index("gx"), lax.axis_index("gy"), lax.axis_index("gz")
    me = gy * NX + gx
    odd = lax.rem(gx, 2)
    near, far = 1 - 2 * odd, 2 * odd - 1

    def shifted(a, b, c):
        return (lax.rem(gx + a + NX, NX), lax.rem(gy + b + NY, NY), lax.rem(gz + c + NZ, NZ))

    def over_planes(action):
        for dy in range(NY):

            def step(dx, carry):
                x, y = lax.rem(gx + dx, NX), lax.rem(gy + dy, NY)
                action(x, y, y * NX + x)
                return carry

            lax.fori_loop(1 if dy == 0 else 0, NX, step, 0)

    barrier = pltpu.get_barrier_semaphore()

    def greet(device):
        pl.semaphore_signal(barrier, inc=1, device_id=device, device_id_type=MESH)

    for c in range(1, NZ):
        greet((gx, gy, lax.rem(gz + c, NZ)))
    over_planes(lambda x, y, p: greet((x, y, gz)))
    for s, a, b, c in LENT:
        greet(shifted(-a, -b, -c))

    feat = feat_ref[...]
    cell = cell_ref[...]
    frac = frac_ref[...].astype(F32)
    up = dot(w_up_ref[...], feat).astype(BF16)
    charge = dot(jnp.broadcast_to(charge_ref[...], (16, CHANNELS)), feat)[0:1, :]
    place[...] = jnp.zeros_like(place)
    place[0:3, :] = cell.astype(F32)
    place[8:11, :] = frac
    spot = place[...]
    export = jnp.concatenate([export_ref[...], export_ref[...]], axis=1)
    pick_t = (lax.broadcasted_iota(jnp.int32, (ATOMS, 128), 0) == export).astype(F32)
    pick = pick_t.T
    ghosts[13, 0:EXPORTED, :] = dot_nt(pick[0:EXPORTED].astype(BF16), up).astype(BF16)
    ghosts[13, EXPORTED : EXPORTED + 16, :] = dot(spot.astype(BF16), pick_t.astype(BF16)).astype(BF16)

    values, slopes = spline_weights(frac)
    along_z = along_z_ref[gz]
    z_waves[...] = dot(
        along_z, node_rows(128, cell[2:3], [v[2:3] for v in values]), HIGHEST
    )
    rows_x = node_rows(16, cell[0:1], [v[0:1] for v in values])
    rows_y = node_rows(24, cell[1:2], [v[1:2] for v in values])
    window[...] = jnp.zeros_like(window)
    for x, half, lane in WINDOWS:
        at = pl.ds(128 * half + lane, HALO_Y)
        window[at, 0:ATOMS] = rows_x[x : x + 1] * rows_y[0:HALO_Y]
    waves = dot_nt(z_waves[...] * charge, window[:, 0:ATOMS], HIGHEST)
    for l in range(NZ):
        parts_out[l] = waves[PLANES * l : PLANES * (l + 1)]

    z_slopes[...] = dot(
        along_z, node_rows(128, cell[2:3], [v[2:3] for v in slopes]), HIGHEST
    )
    slope_x = node_rows(16, cell[0:1], [v[0:1] for v in slopes])
    slope_y = node_rows(24, cell[1:2], [v[1:2] for v in slopes])
    for x, half, lane in WINDOWS:
        at = pl.ds(128 * half + lane, HALO_Y)
        window[at, ATOMS : 2 * ATOMS] = slope_x[x : x + 1] * rows_y[0:HALO_Y]
        window[at, 2 * ATOMS : 3 * ATOMS] = rows_x[x : x + 1] * slope_y[0:HALO_Y]
    entry = neighbor_ref[...]
    lows[...] = entry & 255
    highs[...] = entry >> 8
    sub = lax.broadcasted_iota(jnp.int32, (ATOMS, 2 * ATOMS), 0)

    def two_rows(ref, k):
        return jnp.concatenate([ref[pl.ds(k, 1), :], ref[pl.ds(k + 1, 1), :]], axis=1)

    def heat(pair, carry):
        hots[pair] = jnp.where(sub == two_rows(lows, 2 * pair), 1.0, 0.0).astype(BF16)
        return carry

    lax.fori_loop(0, NEIGHBORS // 2, heat, 0)
    ghosts[27] = jnp.zeros((EXPORTED + 16, 128), BF16)
    table[0, 0:CHANNELS, :] = up
    table[0, CHANNELS:ROWS, :] = spot.astype(BF16)

    pl.semaphore_wait(barrier, (NZ - 1) + (PLANES - 1) + len(LENT))

    def part_copy(c):
        l = lax.rem(gz + c, NZ)
        return pltpu.make_async_remote_copy(
            src_ref=parts_out.at[l],
            dst_ref=parts_in.at[gz],
            send_sem=parts_send.at[c],
            recv_sem=parts_recv.at[NZ - c],
            device_id=(gx, gy, l),
            device_id_type=MESH,
        )

    def part_arrival(c):
        l = lax.rem(gz + c, NZ)
        return pltpu.make_async_remote_copy(
            src_ref=parts_out.at[l],
            dst_ref=parts_in.at[l],
            send_sem=parts_send.at[c],
            recv_sem=parts_recv.at[c],
            device_id=(gx, gy, l),
            device_id_type=MESH,
        )

    def remote(source, target, send, recv, device):
        return pltpu.make_async_remote_copy(
            src_ref=source,
            dst_ref=target,
            send_sem=send,
            recv_sem=recv,
            device_id=device,
            device_id_type=MESH,
        )

    def far_copy(side):
        return remote(
            ghosts.at[13], ghosts.at[9 * (side + 1) + 4], far_send, far_recv, shifted(far, 0, 0)
        )

    def beside_copy(n):
        b, c = BESIDE[n]
        slot = 9 + 3 * (b + 1) + (c + 1)
        return remote(
            ghosts.at[13], ghosts.at[slot], beside_send.at[n], beside_recv.at[n], shifted(0, -b, -c)
        )

    def beyond_copy(n):
        b, c = BESIDE[n]
        slot = 9 * (far + 1) + 3 * (b + 1) + (c + 1)
        return remote(
            ghosts.at[9 * (far + 1) + 4],
            ghosts.at[slot],
            beyond_send.at[n],
            beyond_recv.at[n],
            shifted(0, -b, -c),
        )

    def near_copy(side):
        return remote(
            ghosts.at[pl.ds(9, 9)],
            ghosts.at[pl.ds(9 * (side + 1), 9)],
            near_send,
            near_recv,
            shifted(near, 0, 0),
        )

    far_copy(-far).start()
    for c in range(1, NZ):
        part_copy(c).start()
    for n in range(8):
        beside_copy(n).start()

    parts_in[gz] = parts_out[gz]

    for c in range(1, NZ):
        part_arrival(c).wait_recv()
    total = parts_in[0] + parts_in[1] + parts_in[2] + parts_in[3]
    planes_out[:, 0, :] = total[:, 0:128]
    planes_out[:, 1, :] = total[:, 128:256]

    def plane_copy(x, y, p):
        return pltpu.make_async_remote_copy(
            src_ref=planes_out.at[p],
            dst_ref=planes_in.at[me],
            send_sem=planes_send,
            recv_sem=planes_recv,
            device_id=(x, y, gz),
            device_id_type=MESH,
        )

    over_planes(lambda x, y, p: plane_copy(x, y, p).start())
    planes_in[me] = planes_out[me]

    for n in range(8):
        beside_copy(n).wait_recv()
    near_copy(-near).start()
    far_copy(far).wait_recv()
    for n in range(8):
        beyond_copy(n).start()
    row = lax.broadcasted_iota(jnp.int32, (16, 128), 0)
    lane = lax.broadcasted_iota(jnp.int32, (16, 128), 1)

    def enter(h):
        first = 4 * (h - 1)
        lent = jnp.concatenate([ghosts[first + q, 0:EXPORTED, :] for q in range(4)], axis=0)
        table[h, 0:CHANNELS, :] = lent.astype(F32).T.astype(BF16)
        spots = []
        for q in range(4):
            s = first + q
            a, b, c = s // 9 - 1, lax.rem(s // 3, 3) - 1, lax.rem(s, 3) - 1
            away = jnp.where(
                row == 0, a * CX, jnp.where(row == 1, b * CY, jnp.where(row == 2, c * CZ, 0))
            )
            spots.append(
                ghosts[s, EXPORTED : EXPORTED + 16, :].astype(F32) + away.astype(F32)
            )
        table[h, CHANNELS:ROWS, 0:128] = jnp.where(lane < EXPORTED, spots[0], spots[1]).astype(BF16)
        table[h, CHANNELS:ROWS, 128:256] = jnp.where(lane < EXPORTED, spots[2], spots[3]).astype(BF16)

    near_copy(near).wait_recv()
    soon, late = 4 - 3 * odd, 1 + 4 * odd

    def enter_soon(n, carry):
        enter(soon + n)
        return carry

    lax.fori_loop(0, 4, enter_soon, 0)

    def gather_soon(pair, carry):
        hot = hots[pair]
        gathered[0:ROWS, :] = dot(table[0], hot)
        gathered[ROWS : 5 * ROWS, :] = dot(
            table[pl.ds(soon, 4)].reshape(4 * ROWS, 256), hot
        )
        high8 = jnp.broadcast_to(two_rows(highs, 2 * pair), (8, 2 * ATOMS)) - soon
        for r in range(0, ROWS, 8):
            at = pl.ds(r, 8)
            result = gathered[at, :]
            for n in range(4):
                result = jnp.where(high8 == n, gathered[pl.ds(ROWS * (n + 1) + r, 8), :], result)
            partial[pair, at, :] = result
        return carry

    lax.fori_loop(0, NEIGHBORS // 2, gather_soon, 0)

    weight_high, weight_low = halves(radial_ref[...])
    weights = jnp.concatenate(
        [weight_high, weight_high, weight_low, jnp.zeros((104, CHANNELS), F32)], axis=0
    ).T[:, 0:24].astype(BF16)

    pltpu.make_async_remote_copy(
        src_ref=planes_out.at[pl.ds(0, PLANES - 1)],
        dst_ref=planes_in.at[pl.ds(0, PLANES - 1)],
        send_sem=planes_send,
        recv_sem=planes_recv,
        device_id=(gx, gy, gz),
        device_id_type=MESH,
    ).wait_recv()
    plane = [planes_in[:, 0, :], planes_in[:, 1, :]]
    spread = []
    for x, half, at in WINDOWS:
        line = jnp.zeros((NX, 128), F32)
        for j in range(NY):
            piece = plane[half][NX * j : NX * (j + 1)]
            piece = pltpu.roll(piece, (32 * j - at) % 128, 1)
            inside = jnp.logical_and(lane >= 32 * j, lane < 32 * j + HALO_Y)
            line = jnp.where(inside, piece, line)
        spread.append(line)
    spread.append(jnp.zeros((256 - NX * HALO_X, 128), F32))
    lines = jnp.concatenate(spread, axis=0)
    spectrum = dot(along_x_ref[...], dot(lines, along_yt_ref[...], HIGHEST), HIGHEST)
    mode = gz * PLANES + me
    number = jnp.where(mode <= CZ * NZ // 2, mode, mode - CZ * NZ // 2).astype(F32)
    wave = number * (2.0 * math.pi / (CZ * NZ))
    square = square_ref[...] + wave * wave
    positive = square > 0.0
    safe = jnp.where(positive, square, 1.0)
    filtered = spectrum * jnp.where(
        positive, 4.0 * math.pi * jnp.exp(-square / (4.0 * ewald_beta_sq)) / safe, 0.0
    )
    lines = dot(dot(along_xt_ref[...], filtered, HIGHEST), along_y_ref[...], HIGHEST)
    for j in range(NY):
        for half in range(2):
            piece = jnp.zeros((NX, 128), F32)
            for x, which, at in WINDOWS:
                if which == half:
                    line = pltpu.roll(lines[NX * x : NX * (x + 1)], (at - 32 * j) % 128, 1)
                    inside = jnp.logical_and(lane >= at, lane < at + HALO_Y)
                    piece = jnp.where(inside, line, piece)
            back_out[NX * j : NX * (j + 1), half, :] = piece

    def back_copy(x, y, p):
        return pltpu.make_async_remote_copy(
            src_ref=back_out.at[p],
            dst_ref=back_in.at[me],
            send_sem=back_send,
            recv_sem=back_recv,
            device_id=(x, y, gz),
            device_id_type=MESH,
        )

    over_planes(lambda x, y, p: back_copy(x, y, p).start())
    back_in[me] = back_out[me]

    for n in range(8):
        beyond_copy(n).wait_recv()

    def enter_late(n, carry):
        enter(late + n)
        return carry

    lax.fori_loop(0, 3, enter_late, 0)
    here = spot[0:8] + spot[8:16]
    count = count_ref[...]
    for a in range(4):
        sums[a] = jnp.zeros((CHANNELS, ATOMS), F32)
    centre = lax.broadcasted_iota(jnp.int32, (8, 2 * ATOMS), 0).astype(F32) * basis_step

    def gather(pair, carry):
        k = 2 * pair
        gathered[0 : 3 * ROWS, :] = dot(table[pl.ds(late, 3)].reshape(3 * ROWS, 256), hots[pair])
        high8 = jnp.broadcast_to(two_rows(highs, k), (8, 2 * ATOMS)) - late

        def chosen(start):
            result = partial[pair, pl.ds(start, 8), :]
            for n in range(3):
                result = jnp.where(high8 == n, gathered[pl.ds(start + ROWS * n, 8), :], result)
            return result

        there = chosen(CHANNELS) + chosen(CHANNELS + 8)
        rel = there - jnp.concatenate([here, here], axis=1)
        dist = jnp.sqrt(jnp.sum(rel * rel, axis=0, keepdims=True) + 1.0)
        used = jnp.concatenate([count > k, count > k + 1], axis=1).astype(F32)
        gap = (dist - centre) / basis_width
        basis = jnp.exp(-(gap * gap)) * used
        slope = basis * gap * (-2.0 / basis_width)
        basis_high, basis_low = halves(basis)
        slope_high, slope_low = halves(slope)
        radials[0:CHANNELS, :] = dot(
            weights, jnp.concatenate([basis_high, basis_low, basis_high], axis=0).astype(BF16)
        )
        radials[CHANNELS : 2 * CHANNELS, :] = dot(
            weights, jnp.concatenate([slope_high, slope_low, slope_high], axis=0).astype(BF16)
        )
        inverse = 1.0 / dist
        relatives[k] = rel[:, 0:ATOMS]
        relatives[k + 1] = rel[:, ATOMS:]
        inverses[k] = jnp.broadcast_to(inverse[:, 0:ATOMS], (8, ATOMS))
        inverses[k + 1] = jnp.broadcast_to(inverse[:, ATOMS:], (8, ATOMS))
        along = [jnp.broadcast_to(rel[a : a + 1], (8, 2 * ATOMS)) for a in range(3)]
        for c in range(0, CHANNELS, 8):
            at = pl.ds(c, 8)
            source = chosen(c)
            message = radials[at, :] * source
            turn = radials[pl.ds(CHANNELS + c, 8), :] * source
            messages[k, at, :] = message[:, 0:ATOMS]
            messages[k + 1, at, :] = message[:, ATOMS:]
            turned[k, at, :] = turn[:, 0:ATOMS]
            turned[k + 1, at, :] = turn[:, ATOMS:]
            sums[0, at, :] += message[:, 0:ATOMS] + message[:, ATOMS:]
            for a in range(3):
                moved = message * along[a]
                sums[a + 1, at, :] += moved[:, 0:ATOMS] + moved[:, ATOMS:]
        return carry

    lax.fori_loop(0, NEIGHBORS // 2, gather, 0)

    scalar = sums[0] * message_scale
    vector = [sums[a + 1] * (message_scale * vector_scale) for a in range(3)]
    invariant = scalar + scalar * scalar + (
        vector[0] * vector[0] + vector[1] * vector[1] + vector[2] * vector[2]
    )
    w_out = w_out_ref[...]
    hidden = feat.astype(F32) + dot(w_out, invariant.astype(BF16))
    wide = (
        lax.broadcasted_iota(jnp.int32, (CHANNELS, CHANNELS), 0)
        == lax.broadcasted_iota(jnp.int32, (CHANNELS, CHANNELS), 1)
    ).astype(BF16)
    readout = dot_nt(wide, jnp.broadcast_to(energy_ref[...], (16, CHANNELS)))[:, 0:1]
    gate = 1.0 / (1.0 + jnp.exp(-hidden))
    short = jnp.sum(readout * (hidden * gate), axis=0, keepdims=True)
    d_hidden = readout * (gate * (1.0 + hidden * (1.0 - gate)))
    back_high, back_low = halves(d_hidden)
    w_out_t = w_out.astype(F32).T.astype(BF16)
    d_invariant = dot(w_out_t, back_high.astype(BF16)) + dot(w_out_t, back_low.astype(BF16))
    d_invariant = d_invariant.astype(BF16).astype(F32)
    sums[0] = d_invariant * (1.0 + 2.0 * scalar) * message_scale
    for a in range(3):
        sums[a + 1] = d_invariant * vector[a] * (2.0 * message_scale * vector_scale)

    pltpu.make_async_remote_copy(
        src_ref=back_out.at[pl.ds(0, PLANES - 1)],
        dst_ref=back_in.at[pl.ds(0, PLANES - 1)],
        send_sem=back_send,
        recv_sem=back_recv,
        device_id=(gx, gy, gz),
        device_id_type=MESH,
    ).wait_recv()
    modes[gz, :, 0:128] = back_in[:, 0, :]
    modes[gz, :, 128:256] = back_in[:, 1, :]

    def mode_copy(c):
        return pltpu.make_async_remote_copy(
            src_ref=modes.at[gz],
            dst_ref=modes.at[gz],
            send_sem=modes_send.at[c],
            recv_sem=modes_recv.at[NZ - c],
            device_id=(gx, gy, lax.rem(gz + c, NZ)),
            device_id_type=MESH,
        )

    def mode_arrival(c):
        l = lax.rem(gz + c, NZ)
        return pltpu.make_async_remote_copy(
            src_ref=modes.at[gz],
            dst_ref=modes.at[l],
            send_sem=modes_send.at[c],
            recv_sem=modes_recv.at[c],
            device_id=(gx, gy, l),
            device_id_type=MESH,
        )

    for c in range(1, NZ):
        mode_copy(c).start()

    pushed[...] = jnp.zeros_like(pushed)

    def derive(pair, total):
        k = 2 * pair
        pushes = []
        for e in range(2):
            rel = relatives[k + e]
            along = [jnp.broadcast_to(rel[a : a + 1], (8, ATOMS)) for a in range(3)]
            stretch = jnp.zeros((8, ATOMS), F32)
            direct = [jnp.zeros((8, ATOMS), F32) for _ in range(3)]
            for c in range(0, CHANNELS, 8):
                at = pl.ds(c, 8)
                message = messages[k + e, at, :]
                d_message = sums[0, at, :]
                for a in range(3):
                    d_vector = sums[a + 1, at, :]
                    d_message += d_vector * along[a]
                    direct[a] += d_vector * message
                stretch += d_message * turned[k + e, at, :]
            pull = jnp.sum(stretch, axis=0, keepdims=True) * inverses[k + e][0:1]
            rows = [jnp.sum(direct[a], axis=0, keepdims=True) + pull * rel[a : a + 1] for a in range(3)]
            push = jnp.concatenate(rows + [jnp.zeros((5, ATOMS), F32)], axis=0)
            total = total + push
            pushes.append(push)
        push = jnp.concatenate(pushes, axis=1)
        high = two_rows(highs, k)
        push_high, push_low = halves(push)
        masks = [high == h for h in range(BLOCKS)]
        left = jnp.concatenate(
            [jnp.where(mask, push_high, 0.0) for mask in masks]
            + [jnp.where(mask, push_low, 0.0) for mask in masks],
            axis=0,
        ).astype(BF16)
        pushed[...] += dot_nt(left, hots[pair])
        return total

    pulled = lax.fori_loop(0, NEIGHBORS // 2, derive, jnp.zeros((8, ATOMS), F32))
    reach = pushed[0 : 8 * BLOCKS, :] + pushed[8 * BLOCKS : 16 * BLOCKS, :]
    for s, a, b, c in LENT:
        h, q = s // 4 + 1, s % 4
        piece = reach[8 * h : 8 * (h + 1), 128 * (q // 2) : 128 * (q // 2 + 1)]
        grads_out[s] = (pltpu.roll(piece, 64, 1) if q % 2 else piece)[0:4]

    def grads_copy(s, a, b, c):
        return pltpu.make_async_remote_copy(
            src_ref=grads_out.at[s],
            dst_ref=grads_in.at[s],
            send_sem=grads_send.at[s],
            recv_sem=grads_recv.at[s],
            device_id=shifted(a, b, c),
            device_id_type=MESH,
        )

    for slot in LENT:
        grads_copy(*slot).start()

    for slot in LENT:
        grads_copy(*slot).wait_recv()
    returned = grads_in[LENT[0][0]]
    for slot in LENT[1:]:
        returned = returned + grads_in[slot[0]]
    keep = jnp.where(lax.broadcasted_iota(jnp.int32, (128, ATOMS), 0) < EXPORTED, pick, 0.0)
    returned = jnp.concatenate([returned, jnp.zeros((4, 128), F32)], axis=0)
    grad = reach[0:8] - pulled + dot(returned, keep, HIGHEST)

    for c in range(1, NZ):
        mode_arrival(c).wait_recv()
    field = dot(
        jnp.concatenate([modes[l] for l in range(NZ)], axis=0), window[...], HIGHEST
    )
    here_waves = z_waves[...]
    potential = jnp.sum(here_waves * field[:, 0:ATOMS], axis=0, keepdims=True)
    along_first = jnp.sum(here_waves * field[:, ATOMS : 2 * ATOMS], axis=0, keepdims=True)
    along_second = jnp.sum(here_waves * field[:, 2 * ATOMS :], axis=0, keepdims=True)
    along_third = jnp.sum(z_slopes[...] * field[:, 0:ATOMS], axis=0, keepdims=True)
    forces_ref[0:1, :] = -(grad[0:1] + charge * along_first)
    forces_ref[1:2, :] = -(grad[1:2] + charge * along_second)
    forces_ref[2:3, :] = -(grad[2:3] + charge * along_third)
    atom_energy_ref[...] = short + 0.5 * charge * potential

    for c in range(1, NZ):
        part_copy(c).wait_send()
        mode_copy(c).wait_send()
    far_copy(-far).wait_send()
    near_copy(-near).wait_send()
    for n in range(8):
        beside_copy(n).wait_send()
        beyond_copy(n).wait_send()
    for slot in LENT:
        grads_copy(*slot).wait_send()
    pltpu.make_async_remote_copy(
        src_ref=planes_out.at[pl.ds(0, PLANES - 1)],
        dst_ref=planes_in.at[pl.ds(0, PLANES - 1)],
        send_sem=planes_send,
        recv_sem=planes_recv,
        device_id=(gx, gy, gz),
        device_id_type=MESH,
    ).wait_send()
    pltpu.make_async_remote_copy(
        src_ref=back_out.at[pl.ds(0, PLANES - 1)],
        dst_ref=back_in.at[pl.ds(0, PLANES - 1)],
        send_sem=back_send,
        recv_sem=back_recv,
        device_id=(gx, gy, gz),
        device_id_type=MESH,
    ).wait_send()


def per_device(
    atom_cell,
    atom_frac,
    features,
    ghost_export,
    neighbors,
    neighbor_count,
    w_up,
    radial_weight,
    w_out,
    energy_weight,
    charge_weight,
):
    vmem = pl.BlockSpec(memory_space=pltpu.VMEM)
    constants = tables()
    dma = pltpu.SemaphoreType.DMA
    forces, atom_energy = pl.pallas_call(
        kernel,
        name="layer",
        out_shape=(
            jax.ShapeDtypeStruct((3, ATOMS), F32),
            jax.ShapeDtypeStruct((1, ATOMS), F32),
        ),
        in_specs=[vmem] * (11 + len(constants)),
        out_specs=(vmem, vmem),
        scratch_shapes=[
            pltpu.VMEM((NZ, PLANES, 256), F32),
            pltpu.VMEM((NZ, PLANES, 256), F32),
            pltpu.VMEM((PLANES, 2, 128), F32),
            pltpu.VMEM((PLANES, 2, 128), F32),
            pltpu.VMEM((PLANES, 2, 128), F32),
            pltpu.VMEM((PLANES, 2, 128), F32),
            pltpu.VMEM((NZ, PLANES, 256), F32),
            pltpu.VMEM((28, EXPORTED + 16, 128), BF16),
            pltpu.VMEM((27, 4, 128), F32),
            pltpu.VMEM((27, 4, 128), F32),
            pltpu.VMEM((16, ATOMS), F32),
            pltpu.VMEM((CZ * NZ, ATOMS), F32),
            pltpu.VMEM((CZ * NZ, ATOMS), F32),
            pltpu.VMEM((256, 3 * ATOMS), F32),
            pltpu.VMEM((BLOCKS, ROWS, 256), BF16),
            pltpu.VMEM((5 * ROWS, 2 * ATOMS), F32),
            pltpu.VMEM((NEIGHBORS // 2, ROWS, 2 * ATOMS), F32),
            pltpu.VMEM((2 * CHANNELS, 2 * ATOMS), F32),
            pltpu.VMEM((NEIGHBORS, CHANNELS, ATOMS), F32),
            pltpu.VMEM((NEIGHBORS, CHANNELS, ATOMS), F32),
            pltpu.VMEM((NEIGHBORS // 2, 256, 2 * ATOMS), BF16),
            pltpu.VMEM((NEIGHBORS, ATOMS), jnp.int32),
            pltpu.VMEM((NEIGHBORS, ATOMS), jnp.int32),
            pltpu.VMEM((NEIGHBORS, 8, ATOMS), F32),
            pltpu.VMEM((NEIGHBORS, 8, ATOMS), F32),
            pltpu.VMEM((4, CHANNELS, ATOMS), F32),
            pltpu.VMEM((16 * BLOCKS, 256), F32),
            dma((NZ,)),
            dma((NZ,)),
            dma,
            dma,
            dma,
            dma,
            dma((NZ,)),
            dma((NZ,)),
            dma((8,)),
            dma((8,)),
            dma,
            dma,
            dma((8,)),
            dma((8,)),
            dma,
            dma,
            dma((27,)),
            dma((27,)),
        ],
        compiler_params=pltpu.CompilerParams(collective_id=0, has_side_effects=True),
    )(
        atom_cell,
        atom_frac,
        features,
        ghost_export.reshape(1, EXPORTED),
        neighbors.T,
        neighbor_count.reshape(1, ATOMS),
        w_up,
        radial_weight.T,
        w_out,
        energy_weight.reshape(1, CHANNELS),
        charge_weight.reshape(1, CHANNELS),
        *constants,
    )
    return forces, atom_energy.reshape(ATOMS)


def solution(mesh):
    whole = ("gx", "gy", "gz")
    in_specs = (
        P(None, whole),
        P(None, whole),
        P(None, whole),
        P(whole),
        P(whole, None),
        P(whole),
        P(),
        P(),
        P(),
        P(),
        P(),
    )
    out_specs = (P(None, whole), P(whole))
    return jax.shard_map(
        per_device, mesh=mesh, in_specs=in_specs, out_specs=out_specs, check_vma=False
    )
```

```python
import math

import jax
import jax.numpy as jnp
import numpy as np
from jax import lax
from jax.experimental import pallas as pl
from jax.experimental.pallas import tpu as pltpu
from jax.sharding import PartitionSpec as P

CX, CY, CZ = 8, 16, 64
HALO_X, HALO_Y, HALO_Z = CX + 3, CY + 3, CZ + 3
PER_HALF = 128 // HALO_Y
NX, NY, NZ = 16, 4, 4
PLANES = NX * NY
NEIGHBORS = 32
EXPORTED = 64
ATOMS = 256
CHANNELS = 128
ROWS = CHANNELS + 16
BLOCKS = 8

basis_step = 1.4
basis_width = 1.4
message_scale = 0.125
vector_scale = 1.0 / 6.0
ewald_beta_sq = 2.0

F32 = jnp.float32
BF16 = jnp.bfloat16
MESH = pl.DeviceIdType.MESH
HIGHEST = lax.Precision.HIGHEST

SLOTS = [(s, s // 9 - 1, s // 3 % 3 - 1, s % 3 - 1) for s in range(27)]
LENT = [slot for slot in SLOTS if slot[0] != 13]
BESIDE = [(b, c) for _, a, b, c in LENT if a == 0]
WINDOWS = [(x, x // PER_HALF, HALO_Y * (x % PER_HALF)) for x in range(HALO_X)]


def trig_basis(extent):
    cells = np.arange(extent)
    half = extent // 2
    rows, numbers = [], []
    for k in range(half + 1):
        scale = math.sqrt((1.0 if k in (0, half) else 2.0) / extent)
        rows.append(scale * np.cos(2.0 * math.pi * (k * cells % extent) / extent))
        numbers.append(k)
    for k in range(1, half):
        rows.append(math.sqrt(2.0 / extent) * np.sin(2.0 * math.pi * (k * cells % extent) / extent))
        numbers.append(k)
    return np.array(rows), np.array(numbers)


def tables():
    wave_x, number_x = trig_basis(CX * NX)
    wave_y, number_y = trig_basis(CY * NY)
    wave_z, _ = trig_basis(CZ * NZ)
    along_z = np.zeros((NZ, CZ * NZ, 128), np.float32)
    for l in range(NZ):
        along_z[l, :, :HALO_Z] = wave_z[:, (l * CZ - 1 + np.arange(HALO_Z)) % (CZ * NZ)]
    along_x = np.zeros((CX * NX, 256), np.float32)
    for x in range(HALO_X):
        for i in range(NX):
            along_x[:, x * NX + i] = wave_x[:, (i * CX + x - 1) % (CX * NX)]
    along_y = np.zeros((128, 128), np.float32)
    for j in range(NY):
        for y in range(HALO_Y):
            along_y[: CY * NY, 32 * j + y] = wave_y[:, (j * CY + y - 1) % (CY * NY)]
    square = np.zeros((128, 128), np.float32)
    square[:, : CY * NY] = (2.0 * math.pi / (CX * NX) * number_x[:, None]) ** 2 + (
        2.0 * math.pi / (CY * NY) * number_y[None, :]
    ) ** 2
    square[:, CY * NY :] = 1.0
    return along_z, along_x, along_x.T.copy(), along_y, along_y.T.copy(), square


def spline_weights(t):
    r = 1.0 - t
    t2 = t * t
    t3 = t2 * t
    values = (
        r * r * r / 6.0,
        (3.0 * t3 - 6.0 * t2 + 4.0) / 6.0,
        (-3.0 * t3 + 3.0 * t2 + 3.0 * t + 1.0) / 6.0,
        t3 / 6.0,
    )
    slopes = (-0.5 * r * r, 1.5 * t2 - 2.0 * t, -1.5 * t2 + t + 0.5, 0.5 * t2)
    return values, slopes


def node_rows(count, cell, parts):
    gap = lax.broadcasted_iota(jnp.int32, (count, ATOMS), 0) - cell
    total = jnp.zeros((count, ATOMS), F32)
    for s in range(4):
        total = jnp.where(gap == s, parts[s], total)
    return total


def dot(a, b, precision=None):
    return jnp.dot(a, b, precision=precision, preferred_element_type=F32)


def dot_nt(a, b, precision=None):
    return lax.dot_general(
        a, b, (((1,), (1,)), ((), ())), precision=precision, preferred_element_type=F32
    )


def halves(x):
    high = x.astype(BF16).astype(F32)
    return high, x - high


def kernel(
    cell_ref,
    frac_ref,
    feat_ref,
    export_ref,
    neighbor_ref,
    count_ref,
    w_up_ref,
    radial_ref,
    w_out_ref,
    energy_ref,
    charge_ref,
    along_z_ref,
    along_x_ref,
    along_xt_ref,
    along_y_ref,
    along_yt_ref,
    square_ref,
    forces_ref,
    atom_energy_ref,
    parts_out,
    parts_in,
    planes_out,
    planes_in,
    back_out,
    back_in,
    modes,
    ghosts,
    grads_out,
    grads_in,
    place,
    z_waves,
    z_slopes,
    window,
    table,
    gathered,
    partial,
    radials,
    messages,
    turned,
    hots,
    lows,
    highs,
    relatives,
    sums,
    pushed,
    parts_send,
    parts_recv,
    planes_send,
    planes_recv,
    back_send,
    back_recv,
    modes_send,
    modes_recv,
    beside_send,
    beside_recv,
    far_send,
    far_recv,
    beyond_send,
    beyond_recv,
    near_send,
    near_recv,
    grads_send,
    grads_recv,
):
    gx, gy, gz = lax.axis_index("gx"), lax.axis_index("gy"), lax.axis_index("gz")
    me = gy * NX + gx
    odd = lax.rem(gx, 2)
    near, far = 1 - 2 * odd, 2 * odd - 1

    def shifted(a, b, c):
        return (lax.rem(gx + a + NX, NX), lax.rem(gy + b + NY, NY), lax.rem(gz + c + NZ, NZ))

    def over_planes(action):
        for dy in range(NY):

            def step(dx, carry):
                x, y = lax.rem(gx + dx, NX), lax.rem(gy + dy, NY)
                action(x, y, y * NX + x)
                return carry

            lax.fori_loop(1 if dy == 0 else 0, NX, step, 0)

    barrier = pltpu.get_barrier_semaphore()

    def greet(device):
        pl.semaphore_signal(barrier, inc=1, device_id=device, device_id_type=MESH)

    for c in range(1, NZ):
        greet((gx, gy, lax.rem(gz + c, NZ)))
    over_planes(lambda x, y, p: greet((x, y, gz)))
    for s, a, b, c in LENT:
        greet(shifted(-a, -b, -c))

    feat = feat_ref[...]
    cell = cell_ref[...]
    frac = frac_ref[...].astype(F32)
    up = dot(w_up_ref[...], feat).astype(BF16)
    charge = dot(jnp.broadcast_to(charge_ref[...], (16, CHANNELS)), feat)[0:1, :]
    place[...] = jnp.zeros_like(place)
    place[0:3, :] = cell.astype(F32)
    place[8:11, :] = frac
    spot = place[...]
    export = jnp.concatenate([export_ref[...], export_ref[...]], axis=1)
    pick_t = (lax.broadcasted_iota(jnp.int32, (ATOMS, 128), 0) == export).astype(F32)
    pick = pick_t.T
    ghosts[13, 0:EXPORTED, :] = dot_nt(pick[0:EXPORTED].astype(BF16), up).astype(BF16)
    ghosts[13, EXPORTED : EXPORTED + 16, :] = dot(spot.astype(BF16), pick_t.astype(BF16)).astype(BF16)

    values, slopes = spline_weights(frac)
    along_z = along_z_ref[gz]
    z_waves[...] = dot(
        along_z, node_rows(128, cell[2:3], [v[2:3] for v in values]), HIGHEST
    )
    rows_x = node_rows(16, cell[0:1], [v[0:1] for v in values])
    rows_y = node_rows(24, cell[1:2], [v[1:2] for v in values])
    window[...] = jnp.zeros_like(window)
    for x, half, lane in WINDOWS:
        at = pl.ds(128 * half + lane, HALO_Y)
        window[at, 0:ATOMS] = rows_x[x : x + 1] * rows_y[0:HALO_Y]
    waves = dot_nt(z_waves[...] * charge, window[:, 0:ATOMS], HIGHEST)
    for l in range(NZ):
        parts_out[l] = waves[PLANES * l : PLANES * (l + 1)]

    z_slopes[...] = dot(
        along_z, node_rows(128, cell[2:3], [v[2:3] for v in slopes]), HIGHEST
    )
    slope_x = node_rows(16, cell[0:1], [v[0:1] for v in slopes])
    slope_y = node_rows(24, cell[1:2], [v[1:2] for v in slopes])
    for x, half, lane in WINDOWS:
        at = pl.ds(128 * half + lane, HALO_Y)
        window[at, ATOMS : 2 * ATOMS] = slope_x[x : x + 1] * rows_y[0:HALO_Y]
        window[at, 2 * ATOMS : 3 * ATOMS] = rows_x[x : x + 1] * slope_y[0:HALO_Y]
    entry = neighbor_ref[...]
    lows[...] = entry & 255
    highs[...] = entry >> 8
    sub = lax.broadcasted_iota(jnp.int32, (ATOMS, 2 * ATOMS), 0)

    def two_rows(ref, k):
        return jnp.concatenate([ref[pl.ds(k, 1), :], ref[pl.ds(k + 1, 1), :]], axis=1)

    ghosts[27] = jnp.zeros((EXPORTED + 16, 128), BF16)
    table[0, 0:CHANNELS, :] = up
    table[0, CHANNELS:ROWS, :] = spot.astype(BF16)

    def gather_own(pair, carry):
        hot = jnp.where(sub == two_rows(lows, 2 * pair), 1.0, 0.0).astype(BF16)
        hots[pair] = hot
        partial[pair] = dot(table[0, 0:ROWS, :], hot).astype(BF16)
        return carry

    lax.fori_loop(0, NEIGHBORS // 2, gather_own, 0)

    pl.semaphore_wait(barrier, (NZ - 1) + (PLANES - 1) + len(LENT))

    def part_copy(c):
        l = lax.rem(gz + c, NZ)
        return pltpu.make_async_remote_copy(
            src_ref=parts_out.at[l],
            dst_ref=parts_in.at[gz],
            send_sem=parts_send.at[c],
            recv_sem=parts_recv.at[NZ - c],
            device_id=(gx, gy, l),
            device_id_type=MESH,
        )

    def part_arrival(c):
        l = lax.rem(gz + c, NZ)
        return pltpu.make_async_remote_copy(
            src_ref=parts_out.at[l],
            dst_ref=parts_in.at[l],
            send_sem=parts_send.at[c],
            recv_sem=parts_recv.at[c],
            device_id=(gx, gy, l),
            device_id_type=MESH,
        )

    def remote(source, target, send, recv, device):
        return pltpu.make_async_remote_copy(
            src_ref=source,
            dst_ref=target,
            send_sem=send,
            recv_sem=recv,
            device_id=device,
            device_id_type=MESH,
        )

    def far_copy(side):
        return remote(
            ghosts.at[13], ghosts.at[9 * (side + 1) + 4], far_send, far_recv, shifted(far, 0, 0)
        )

    def beside_copy(n):
        b, c = BESIDE[n]
        slot = 9 + 3 * (b + 1) + (c + 1)
        return remote(
            ghosts.at[13], ghosts.at[slot], beside_send.at[n], beside_recv.at[n], shifted(0, -b, -c)
        )

    def beyond_copy(n):
        b, c = BESIDE[n]
        slot = 9 * (far + 1) + 3 * (b + 1) + (c + 1)
        return remote(
            ghosts.at[9 * (far + 1) + 4],
            ghosts.at[slot],
            beyond_send.at[n],
            beyond_recv.at[n],
            shifted(0, -b, -c),
        )

    def near_copy(side):
        return remote(
            ghosts.at[pl.ds(9, 9)],
            ghosts.at[pl.ds(9 * (side + 1), 9)],
            near_send,
            near_recv,
            shifted(near, 0, 0),
        )

    far_copy(-far).start()
    for c in range(1, NZ):
        part_copy(c).start()
    for n in range(8):
        beside_copy(n).start()

    parts_in[gz] = parts_out[gz]

    for c in range(1, NZ):
        part_arrival(c).wait_recv()
    total = parts_in[0] + parts_in[1] + parts_in[2] + parts_in[3]
    planes_out[:, 0, :] = total[:, 0:128]
    planes_out[:, 1, :] = total[:, 128:256]

    def plane_copy(x, y, p):
        return pltpu.make_async_remote_copy(
            src_ref=planes_out.at[p],
            dst_ref=planes_in.at[me],
            send_sem=planes_send,
            recv_sem=planes_recv,
            device_id=(x, y, gz),
            device_id_type=MESH,
        )

    over_planes(lambda x, y, p: plane_copy(x, y, p).start())
    planes_in[me] = planes_out[me]

    for n in range(8):
        beside_copy(n).wait_recv()
    near_copy(-near).start()
    far_copy(far).wait_recv()
    for n in range(8):
        beyond_copy(n).start()
    row = lax.broadcasted_iota(jnp.int32, (16, 128), 0)
    lane = lax.broadcasted_iota(jnp.int32, (16, 128), 1)

    def enter(h):
        first = 4 * (h - 1)
        lent = jnp.concatenate([ghosts[first + q, 0:EXPORTED, :] for q in range(4)], axis=0)
        table[h, 0:CHANNELS, :] = lent.astype(F32).T.astype(BF16)
        spots = []
        for q in range(4):
            s = first + q
            a, b, c = s // 9 - 1, lax.rem(s // 3, 3) - 1, lax.rem(s, 3) - 1
            away = jnp.where(
                row == 0, a * CX, jnp.where(row == 1, b * CY, jnp.where(row == 2, c * CZ, 0))
            )
            spots.append(
                ghosts[s, EXPORTED : EXPORTED + 16, :].astype(F32) + away.astype(F32)
            )
        table[h, CHANNELS:ROWS, 0:128] = jnp.where(lane < EXPORTED, spots[0], spots[1]).astype(BF16)
        table[h, CHANNELS:ROWS, 128:256] = jnp.where(lane < EXPORTED, spots[2], spots[3]).astype(BF16)

    near_copy(near).wait_recv()
    soon, late = 4 - 3 * odd, 1 + 4 * odd

    def enter_soon(n, carry):
        enter(soon + n)
        return carry

    lax.fori_loop(0, 4, enter_soon, 0)

    def blocks_of(k, first):
        block = (two_rows(highs, k) - first).astype(F32)
        return jnp.broadcast_to(block, (16, 2 * ATOMS)).astype(BF16)

    def gather_soon(pair, carry):
        gathered[...] = dot(
            table[pl.ds(soon, 4), 0:ROWS, :].reshape(4 * ROWS, 256), hots[pair]
        ).astype(BF16)
        block = blocks_of(2 * pair, soon)
        for r in range(0, ROWS, 16):
            at = pl.ds(r, 16)
            result = partial[pair, at, :]
            for n in range(4):
                result = jnp.where(block == n, gathered[pl.ds(ROWS * n + r, 16), :], result)
            partial[pair, at, :] = result
        return carry

    lax.fori_loop(0, NEIGHBORS // 2, gather_soon, 0)

    weight_high, weight_low = halves(radial_ref[...])
    weights = jnp.concatenate(
        [weight_high, weight_high, weight_low, jnp.zeros((104, CHANNELS), F32)], axis=0
    ).T[:, 0:24].astype(BF16)

    for n in range(8):
        beyond_copy(n).wait_recv()

    def enter_late(n, carry):
        enter(late + n)
        return carry

    lax.fori_loop(0, 3, enter_late, 0)
    here = spot[0:8] + spot[8:16]
    count = count_ref[...]
    for a in range(4):
        sums[a] = jnp.zeros((CHANNELS, ATOMS), F32)
    centre = lax.broadcasted_iota(jnp.int32, (8, 2 * ATOMS), 0).astype(F32) * basis_step

    def gather(pair, carry):
        k = 2 * pair
        gathered[0 : 3 * ROWS, :] = dot(
            table[pl.ds(late, 3), 0:ROWS, :].reshape(3 * ROWS, 256), hots[pair]
        ).astype(BF16)
        block = blocks_of(k, late)

        def chosen(start):
            result = partial[pair, pl.ds(start, 16), :]
            for n in range(3):
                result = jnp.where(block == n, gathered[pl.ds(start + ROWS * n, 16), :], result)
            return result.astype(F32)

        there = chosen(CHANNELS)
        there = there[0:8] + there[8:16]
        rel = there - jnp.concatenate([here, here], axis=1)
        dist = jnp.sqrt(jnp.sum(rel * rel, axis=0, keepdims=True) + 1.0)
        used = jnp.concatenate([count > k, count > k + 1], axis=1).astype(F32)
        gap = (dist - centre) / basis_width
        basis = jnp.exp(-(gap * gap)) * used
        slope = basis * gap * (-2.0 / basis_width)
        basis_high, basis_low = halves(basis)
        slope_high, slope_low = halves(slope)
        radials[0:CHANNELS, :] = dot(
            weights, jnp.concatenate([basis_high, basis_low, basis_high], axis=0).astype(BF16)
        )
        radials[CHANNELS : 2 * CHANNELS, :] = dot(
            weights, jnp.concatenate([slope_high, slope_low, slope_high], axis=0).astype(BF16)
        )
        inverse = 1.0 / dist
        relatives[k, 0:8, :] = rel[:, 0:ATOMS]
        relatives[k + 1, 0:8, :] = rel[:, ATOMS:]
        relatives[k, 8:16, :] = jnp.broadcast_to(inverse[:, 0:ATOMS], (8, ATOMS))
        relatives[k + 1, 8:16, :] = jnp.broadcast_to(inverse[:, ATOMS:], (8, ATOMS))
        along = [jnp.broadcast_to(rel[a : a + 1], (8, 2 * ATOMS)) for a in range(3)]
        for c in range(0, CHANNELS, 16):
            sources = chosen(c)
            for half in range(2):
                at = pl.ds(c + 8 * half, 8)
                source = sources[8 * half : 8 * (half + 1)]
                message = radials[at, :] * source
                turn = radials[pl.ds(CHANNELS + c + 8 * half, 8), :] * source
                messages[k, at, :] = message[:, 0:ATOMS]
                messages[k + 1, at, :] = message[:, ATOMS:]
                turned[k, at, :] = turn[:, 0:ATOMS]
                turned[k + 1, at, :] = turn[:, ATOMS:]
                sums[0, at, :] += message[:, 0:ATOMS] + message[:, ATOMS:]
                for a in range(3):
                    moved = message * along[a]
                    sums[a + 1, at, :] += moved[:, 0:ATOMS] + moved[:, ATOMS:]
        return carry

    lax.fori_loop(0, NEIGHBORS // 4, gather, 0)

    pltpu.make_async_remote_copy(
        src_ref=planes_out.at[pl.ds(0, PLANES - 1)],
        dst_ref=planes_in.at[pl.ds(0, PLANES - 1)],
        send_sem=planes_send,
        recv_sem=planes_recv,
        device_id=(gx, gy, gz),
        device_id_type=MESH,
    ).wait_recv()
    plane = [planes_in[:, 0, :], planes_in[:, 1, :]]
    spread = []
    for x, half, at in WINDOWS:
        line = jnp.zeros((NX, 128), F32)
        for j in range(NY):
            piece = plane[half][NX * j : NX * (j + 1)]
            piece = pltpu.roll(piece, (32 * j - at) % 128, 1)
            inside = jnp.logical_and(lane >= 32 * j, lane < 32 * j + HALO_Y)
            line = jnp.where(inside, piece, line)
        spread.append(line)
    spread.append(jnp.zeros((256 - NX * HALO_X, 128), F32))
    lines = jnp.concatenate(spread, axis=0)
    spectrum = dot(along_x_ref[...], dot(lines, along_yt_ref[...], HIGHEST), HIGHEST)
    mode = gz * PLANES + me
    number = jnp.where(mode <= CZ * NZ // 2, mode, mode - CZ * NZ // 2).astype(F32)
    wave = number * (2.0 * math.pi / (CZ * NZ))
    square = square_ref[...] + wave * wave
    positive = square > 0.0
    safe = jnp.where(positive, square, 1.0)
    filtered = spectrum * jnp.where(
        positive, 4.0 * math.pi * jnp.exp(-square / (4.0 * ewald_beta_sq)) / safe, 0.0
    )
    lines = dot(dot(along_xt_ref[...], filtered, HIGHEST), along_y_ref[...], HIGHEST)
    for j in range(NY):
        for half in range(2):
            piece = jnp.zeros((NX, 128), F32)
            for x, which, at in WINDOWS:
                if which == half:
                    line = pltpu.roll(lines[NX * x : NX * (x + 1)], (at - 32 * j) % 128, 1)
                    inside = jnp.logical_and(lane >= at, lane < at + HALO_Y)
                    piece = jnp.where(inside, line, piece)
            back_out[NX * j : NX * (j + 1), half, :] = piece

    def back_copy(x, y, p):
        return pltpu.make_async_remote_copy(
            src_ref=back_out.at[p],
            dst_ref=back_in.at[me],
            send_sem=back_send,
            recv_sem=back_recv,
            device_id=(x, y, gz),
            device_id_type=MESH,
        )

    over_planes(lambda x, y, p: back_copy(x, y, p).start())
    back_in[me] = back_out[me]

    lax.fori_loop(NEIGHBORS // 4, NEIGHBORS // 2, gather, 0)

    scalar = sums[0] * message_scale
    vector = [sums[a + 1] * (message_scale * vector_scale) for a in range(3)]
    invariant = scalar + scalar * scalar + (
        vector[0] * vector[0] + vector[1] * vector[1] + vector[2] * vector[2]
    )
    w_out = w_out_ref[...]
    hidden = feat.astype(F32) + dot(w_out, invariant.astype(BF16))
    wide = (
        lax.broadcasted_iota(jnp.int32, (CHANNELS, CHANNELS), 0)
        == lax.broadcasted_iota(jnp.int32, (CHANNELS, CHANNELS), 1)
    ).astype(BF16)
    readout = dot_nt(wide, jnp.broadcast_to(energy_ref[...], (16, CHANNELS)))[:, 0:1]
    gate = 1.0 / (1.0 + jnp.exp(-hidden))
    short = jnp.sum(readout * (hidden * gate), axis=0, keepdims=True)
    d_hidden = readout * (gate * (1.0 + hidden * (1.0 - gate)))
    back_high, back_low = halves(d_hidden)
    w_out_t = w_out.astype(F32).T.astype(BF16)
    d_invariant = dot(w_out_t, back_high.astype(BF16)) + dot(w_out_t, back_low.astype(BF16))
    d_invariant = d_invariant.astype(BF16).astype(F32)
    sums[0] = d_invariant * (1.0 + 2.0 * scalar) * message_scale
    for a in range(3):
        sums[a + 1] = d_invariant * vector[a] * (2.0 * message_scale * vector_scale)

    pushed[...] = jnp.zeros_like(pushed)

    def derive(pair, total):
        k = 2 * pair
        rel = [relatives[k + e, 0:8, :] for e in range(2)]
        along = [[jnp.broadcast_to(rel[e][a : a + 1], (8, ATOMS)) for a in range(3)] for e in range(2)]
        stretch = [jnp.zeros((8, ATOMS), F32) for _ in range(2)]
        direct = [[jnp.zeros((8, ATOMS), F32) for _ in range(3)] for _ in range(2)]
        for c in range(0, CHANNELS, 8):
            at = pl.ds(c, 8)
            d_scalar = sums[0, at, :]
            d_vector = [sums[a + 1, at, :] for a in range(3)]
            for e in range(2):
                message = messages[k + e, at, :]
                d_message = d_scalar
                for a in range(3):
                    d_message += d_vector[a] * along[e][a]
                    direct[e][a] += d_vector[a] * message
                stretch[e] += d_message * turned[k + e, at, :]
        pushes = []
        for e in range(2):
            pull = jnp.sum(stretch[e], axis=0, keepdims=True) * relatives[k + e, 8:9, :]
            rows = [
                jnp.sum(direct[e][a], axis=0, keepdims=True) + pull * rel[e][a : a + 1]
                for a in range(3)
            ]
            push = jnp.concatenate(rows + [jnp.zeros((5, ATOMS), F32)], axis=0)
            total = total + push
            pushes.append(push)
        push = jnp.concatenate(pushes, axis=1)
        high = two_rows(highs, k)
        push_high, push_low = halves(push)
        masks = [high == h for h in range(BLOCKS)]
        left = jnp.concatenate(
            [jnp.where(mask, push_high, 0.0) for mask in masks]
            + [jnp.where(mask, push_low, 0.0) for mask in masks],
            axis=0,
        ).astype(BF16)
        pushed[...] += dot_nt(left, hots[pair])
        return total

    pulled = lax.fori_loop(0, NEIGHBORS // 8, derive, jnp.zeros((8, ATOMS), F32))

    pltpu.make_async_remote_copy(
        src_ref=back_out.at[pl.ds(0, PLANES - 1)],
        dst_ref=back_in.at[pl.ds(0, PLANES - 1)],
        send_sem=back_send,
        recv_sem=back_recv,
        device_id=(gx, gy, gz),
        device_id_type=MESH,
    ).wait_recv()
    modes[gz, :, 0:128] = back_in[:, 0, :]
    modes[gz, :, 128:256] = back_in[:, 1, :]

    def mode_copy(c):
        return pltpu.make_async_remote_copy(
            src_ref=modes.at[gz],
            dst_ref=modes.at[gz],
            send_sem=modes_send.at[c],
            recv_sem=modes_recv.at[NZ - c],
            device_id=(gx, gy, lax.rem(gz + c, NZ)),
            device_id_type=MESH,
        )

    def mode_arrival(c):
        l = lax.rem(gz + c, NZ)
        return pltpu.make_async_remote_copy(
            src_ref=modes.at[gz],
            dst_ref=modes.at[l],
            send_sem=modes_send.at[c],
            recv_sem=modes_recv.at[c],
            device_id=(gx, gy, l),
            device_id_type=MESH,
        )

    for c in range(1, NZ):
        mode_copy(c).start()

    pulled = lax.fori_loop(NEIGHBORS // 8, NEIGHBORS // 2, derive, pulled)
    reach = pushed[0 : 8 * BLOCKS, :] + pushed[8 * BLOCKS : 16 * BLOCKS, :]
    for s, a, b, c in LENT:
        h, q = s // 4 + 1, s % 4
        piece = reach[8 * h : 8 * (h + 1), 128 * (q // 2) : 128 * (q // 2 + 1)]
        grads_out[s] = (pltpu.roll(piece, 64, 1) if q % 2 else piece)[0:4]

    def grads_copy(s, a, b, c):
        return pltpu.make_async_remote_copy(
            src_ref=grads_out.at[s],
            dst_ref=grads_in.at[s],
            send_sem=grads_send.at[s],
            recv_sem=grads_recv.at[s],
            device_id=shifted(a, b, c),
            device_id_type=MESH,
        )

    for slot in LENT:
        grads_copy(*slot).start()

    for c in range(1, NZ):
        mode_arrival(c).wait_recv()
    field = dot(
        jnp.concatenate([modes[l] for l in range(NZ)], axis=0), window[...], HIGHEST
    )
    here_waves = z_waves[...]
    potential = jnp.sum(here_waves * field[:, 0:ATOMS], axis=0, keepdims=True)
    along_first = jnp.sum(here_waves * field[:, ATOMS : 2 * ATOMS], axis=0, keepdims=True)
    along_second = jnp.sum(here_waves * field[:, 2 * ATOMS :], axis=0, keepdims=True)
    along_third = jnp.sum(z_slopes[...] * field[:, 0:ATOMS], axis=0, keepdims=True)
    atom_energy_ref[...] = short + 0.5 * charge * potential
    for slot in LENT:
        grads_copy(*slot).wait_recv()
    returned = grads_in[LENT[0][0]]
    for slot in LENT[1:]:
        returned = returned + grads_in[slot[0]]
    keep = jnp.where(lax.broadcasted_iota(jnp.int32, (128, ATOMS), 0) < EXPORTED, pick, 0.0)
    returned = jnp.concatenate([returned, jnp.zeros((4, 128), F32)], axis=0)
    grad = reach[0:8] - pulled + dot(returned, keep, HIGHEST)

    forces_ref[0:1, :] = -(grad[0:1] + charge * along_first)
    forces_ref[1:2, :] = -(grad[1:2] + charge * along_second)
    forces_ref[2:3, :] = -(grad[2:3] + charge * along_third)

    for c in range(1, NZ):
        part_copy(c).wait_send()
        mode_copy(c).wait_send()
    far_copy(-far).wait_send()
    near_copy(-near).wait_send()
    for n in range(8):
        beside_copy(n).wait_send()
        beyond_copy(n).wait_send()
    for slot in LENT:
        grads_copy(*slot).wait_send()
    pltpu.make_async_remote_copy(
        src_ref=planes_out.at[pl.ds(0, PLANES - 1)],
        dst_ref=planes_in.at[pl.ds(0, PLANES - 1)],
        send_sem=planes_send,
        recv_sem=planes_recv,
        device_id=(gx, gy, gz),
        device_id_type=MESH,
    ).wait_send()
    pltpu.make_async_remote_copy(
        src_ref=back_out.at[pl.ds(0, PLANES - 1)],
        dst_ref=back_in.at[pl.ds(0, PLANES - 1)],
        send_sem=back_send,
        recv_sem=back_recv,
        device_id=(gx, gy, gz),
        device_id_type=MESH,
    ).wait_send()


def per_device(
    atom_cell,
    atom_frac,
    features,
    ghost_export,
    neighbors,
    neighbor_count,
    w_up,
    radial_weight,
    w_out,
    energy_weight,
    charge_weight,
):
    vmem = pl.BlockSpec(memory_space=pltpu.VMEM)
    constants = tables()
    dma = pltpu.SemaphoreType.DMA
    forces, atom_energy = pl.pallas_call(
        kernel,
        name="layer",
        out_shape=(
            pltpu.VMEM((3, ATOMS), F32),
            pltpu.VMEM((1, ATOMS), F32),
        ),
        in_specs=[vmem] * (11 + len(constants)),
        out_specs=(vmem, vmem),
        scratch_shapes=[
            pltpu.VMEM((NZ, PLANES, 256), F32),
            pltpu.VMEM((NZ, PLANES, 256), F32),
            pltpu.VMEM((PLANES, 2, 128), F32),
            pltpu.VMEM((PLANES, 2, 128), F32),
            pltpu.VMEM((PLANES, 2, 128), F32),
            pltpu.VMEM((PLANES, 2, 128), F32),
            pltpu.VMEM((NZ, PLANES, 256), F32),
            pltpu.VMEM((28, EXPORTED + 16, 128), BF16),
            pltpu.VMEM((32, 4, 128), F32),
            pltpu.VMEM((32, 4, 128), F32),
            pltpu.VMEM((16, ATOMS), F32),
            pltpu.VMEM((CZ * NZ, ATOMS), F32),
            pltpu.VMEM((CZ * NZ, ATOMS), F32),
            pltpu.VMEM((256, 3 * ATOMS), F32),
            pltpu.VMEM((BLOCKS, CHANNELS + 32, 256), BF16),
            pltpu.VMEM((4 * ROWS, 2 * ATOMS), BF16),
            pltpu.VMEM((NEIGHBORS // 2, ROWS, 2 * ATOMS), BF16),
            pltpu.VMEM((2 * CHANNELS, 2 * ATOMS), F32),
            pltpu.VMEM((NEIGHBORS, CHANNELS, ATOMS), F32),
            pltpu.VMEM((NEIGHBORS, CHANNELS, ATOMS), F32),
            pltpu.VMEM((NEIGHBORS // 2, 256, 2 * ATOMS), BF16),
            pltpu.VMEM((NEIGHBORS, ATOMS), jnp.int32),
            pltpu.VMEM((NEIGHBORS, ATOMS), jnp.int32),
            pltpu.VMEM((NEIGHBORS, 16, ATOMS), F32),
            pltpu.VMEM((4, CHANNELS, ATOMS), F32),
            pltpu.VMEM((16 * BLOCKS, 256), F32),
            dma((NZ,)),
            dma((NZ,)),
            dma,
            dma,
            dma,
            dma,
            dma((NZ,)),
            dma((NZ,)),
            dma((8,)),
            dma((8,)),
            dma,
            dma,
            dma((8,)),
            dma((8,)),
            dma,
            dma,
            dma((27,)),
            dma((27,)),
        ],
        compiler_params=pltpu.CompilerParams(collective_id=0, has_side_effects=True),
    )(
        atom_cell,
        atom_frac,
        features,
        ghost_export.reshape(1, EXPORTED),
        neighbors.T,
        neighbor_count.reshape(1, ATOMS),
        w_up,
        radial_weight.T,
        w_out,
        energy_weight.reshape(1, CHANNELS),
        charge_weight.reshape(1, CHANNELS),
        *constants,
    )
    return forces, atom_energy.reshape(ATOMS)


def solution(mesh):
    whole = ("gx", "gy", "gz")
    in_specs = (
        P(None, whole),
        P(None, whole),
        P(None, whole),
        P(whole),
        P(whole, None),
        P(whole),
        P(),
        P(),
        P(),
        P(),
        P(),
    )
    out_specs = (P(None, whole), P(whole))
    return jax.shard_map(
        per_device, mesh=mesh, in_specs=in_specs, out_specs=out_specs, check_vma=False
    )
```

```python
import math

import jax
import jax.numpy as jnp
import numpy as np
from jax import lax
from jax.experimental import pallas as pl
from jax.experimental.pallas import tpu as pltpu
from jax.sharding import PartitionSpec as P

CX, CY, CZ = 8, 16, 64
HALO_X, HALO_Y, HALO_Z = CX + 3, CY + 3, CZ + 3
PER_HALF = 128 // HALO_Y
NX, NY, NZ = 16, 4, 4
PLANES = NX * NY
NEIGHBORS = 32
EXPORTED = 64
ATOMS = 256
CHANNELS = 128
ROWS = CHANNELS + 16
BLOCKS = 8

basis_step = 1.4
basis_width = 1.4
message_scale = 0.125
vector_scale = 1.0 / 6.0
ewald_beta_sq = 2.0

F32 = jnp.float32
BF16 = jnp.bfloat16
MESH = pl.DeviceIdType.MESH
HIGHEST = lax.Precision.HIGHEST

SLOTS = [(s, s // 9 - 1, s // 3 % 3 - 1, s % 3 - 1) for s in range(27)]
LENT = [slot for slot in SLOTS if slot[0] != 13]
BESIDE = [(b, c) for _, a, b, c in LENT if a == 0]
WINDOWS = [(x, x // PER_HALF, HALO_Y * (x % PER_HALF)) for x in range(HALO_X)]


def trig_basis(extent):
    cells = np.arange(extent)
    half = extent // 2
    rows, numbers = [], []
    for k in range(half + 1):
        scale = math.sqrt((1.0 if k in (0, half) else 2.0) / extent)
        rows.append(scale * np.cos(2.0 * math.pi * (k * cells % extent) / extent))
        numbers.append(k)
    for k in range(1, half):
        rows.append(math.sqrt(2.0 / extent) * np.sin(2.0 * math.pi * (k * cells % extent) / extent))
        numbers.append(k)
    return np.array(rows), np.array(numbers)


def tables():
    wave_x, number_x = trig_basis(CX * NX)
    wave_y, number_y = trig_basis(CY * NY)
    wave_z, _ = trig_basis(CZ * NZ)
    along_z = np.zeros((NZ, CZ * NZ, 128), np.float32)
    for l in range(NZ):
        along_z[l, :, :HALO_Z] = wave_z[:, (l * CZ - 1 + np.arange(HALO_Z)) % (CZ * NZ)]
    along_x = np.zeros((CX * NX, 256), np.float32)
    for x in range(HALO_X):
        for i in range(NX):
            along_x[:, x * NX + i] = wave_x[:, (i * CX + x - 1) % (CX * NX)]
    along_y = np.zeros((128, 128), np.float32)
    for j in range(NY):
        for y in range(HALO_Y):
            along_y[: CY * NY, 32 * j + y] = wave_y[:, (j * CY + y - 1) % (CY * NY)]
    square = np.zeros((128, 128), np.float32)
    square[:, : CY * NY] = (2.0 * math.pi / (CX * NX) * number_x[:, None]) ** 2 + (
        2.0 * math.pi / (CY * NY) * number_y[None, :]
    ) ** 2
    square[:, CY * NY :] = 1.0
    return along_z, along_x, along_x.T.copy(), along_y, along_y.T.copy(), square


def spline_weights(t):
    r = 1.0 - t
    t2 = t * t
    t3 = t2 * t
    values = (
        r * r * r / 6.0,
        (3.0 * t3 - 6.0 * t2 + 4.0) / 6.0,
        (-3.0 * t3 + 3.0 * t2 + 3.0 * t + 1.0) / 6.0,
        t3 / 6.0,
    )
    slopes = (-0.5 * r * r, 1.5 * t2 - 2.0 * t, -1.5 * t2 + t + 0.5, 0.5 * t2)
    return values, slopes


def node_rows(count, cell, parts):
    gap = lax.broadcasted_iota(jnp.int32, (count, ATOMS), 0) - cell
    total = jnp.zeros((count, ATOMS), F32)
    for s in range(4):
        total = jnp.where(gap == s, parts[s], total)
    return total


def dot(a, b, precision=None):
    return jnp.dot(a, b, precision=precision, preferred_element_type=F32)


def dot_nt(a, b, precision=None):
    return lax.dot_general(
        a, b, (((1,), (1,)), ((), ())), precision=precision, preferred_element_type=F32
    )


def halves(x):
    high = x.astype(BF16).astype(F32)
    return high, x - high


def kernel(
    cell_ref,
    frac_ref,
    feat_ref,
    export_ref,
    neighbor_ref,
    count_ref,
    w_up_ref,
    radial_ref,
    w_out_ref,
    energy_ref,
    charge_ref,
    along_z_ref,
    along_x_ref,
    along_xt_ref,
    along_y_ref,
    along_yt_ref,
    square_ref,
    forces_ref,
    atom_energy_ref,
    parts_out,
    parts_in,
    planes_out,
    planes_in,
    back_out,
    back_in,
    modes,
    ghosts,
    grads_out,
    grads_in,
    place,
    z_waves,
    z_slopes,
    window,
    table,
    gathered,
    partial,
    radials,
    messages,
    turned,
    hots,
    lows,
    highs,
    relatives,
    inverses,
    sums,
    pushed,
    parts_send,
    parts_recv,
    planes_send,
    planes_recv,
    back_send,
    back_recv,
    modes_send,
    modes_recv,
    beside_send,
    beside_recv,
    far_send,
    far_recv,
    beyond_send,
    beyond_recv,
    near_send,
    near_recv,
    grads_send,
    grads_recv,
):
    gx, gy, gz = lax.axis_index("gx"), lax.axis_index("gy"), lax.axis_index("gz")
    me = gy * NX + gx
    odd = lax.rem(gx, 2)
    near, far = 1 - 2 * odd, 2 * odd - 1

    def shifted(a, b, c):
        return (lax.rem(gx + a + NX, NX), lax.rem(gy + b + NY, NY), lax.rem(gz + c + NZ, NZ))

    def over_planes(action):
        for dy in range(NY):

            def step(dx, carry):
                x, y = lax.rem(gx + dx, NX), lax.rem(gy + dy, NY)
                action(x, y, y * NX + x)
                return carry

            lax.fori_loop(1 if dy == 0 else 0, NX, step, 0)

    barrier = pltpu.get_barrier_semaphore()

    def greet(device):
        pl.semaphore_signal(barrier, inc=1, device_id=device, device_id_type=MESH)

    for c in range(1, NZ):
        greet((gx, gy, lax.rem(gz + c, NZ)))
    over_planes(lambda x, y, p: greet((x, y, gz)))
    for s, a, b, c in LENT:
        greet(shifted(-a, -b, -c))

    feat = feat_ref[...]
    cell = cell_ref[...]
    frac = frac_ref[...].astype(F32)
    up = dot(w_up_ref[...], feat).astype(BF16)
    charge = dot(jnp.broadcast_to(charge_ref[...], (16, CHANNELS)), feat)[0:1, :]
    place[...] = jnp.zeros_like(place)
    place[0:3, :] = cell.astype(F32)
    place[8:11, :] = frac
    spot = place[...]
    export = jnp.concatenate([export_ref[...], export_ref[...]], axis=1)
    pick_t = (lax.broadcasted_iota(jnp.int32, (ATOMS, 128), 0) == export).astype(F32)
    pick = pick_t.T
    ghosts[13, 0:EXPORTED, :] = dot_nt(pick[0:EXPORTED].astype(BF16), up).astype(BF16)
    ghosts[13, EXPORTED : EXPORTED + 16, :] = dot(spot.astype(BF16), pick_t.astype(BF16)).astype(BF16)

    values, slopes = spline_weights(frac)
    along_z = along_z_ref[gz]
    z_waves[...] = dot(
        along_z, node_rows(128, cell[2:3], [v[2:3] for v in values]), HIGHEST
    )
    rows_x = node_rows(16, cell[0:1], [v[0:1] for v in values])
    rows_y = node_rows(24, cell[1:2], [v[1:2] for v in values])
    window[...] = jnp.zeros_like(window)
    for x, half, lane in WINDOWS:
        at = pl.ds(128 * half + lane, HALO_Y)
        window[at, 0:ATOMS] = rows_x[x : x + 1] * rows_y[0:HALO_Y]
    waves = dot_nt(z_waves[...] * charge, window[:, 0:ATOMS], HIGHEST)
    for l in range(NZ):
        parts_out[l] = waves[PLANES * l : PLANES * (l + 1)]

    z_slopes[...] = dot(
        along_z, node_rows(128, cell[2:3], [v[2:3] for v in slopes]), HIGHEST
    )
    slope_x = node_rows(16, cell[0:1], [v[0:1] for v in slopes])
    slope_y = node_rows(24, cell[1:2], [v[1:2] for v in slopes])
    for x, half, lane in WINDOWS:
        at = pl.ds(128 * half + lane, HALO_Y)
        window[at, ATOMS : 2 * ATOMS] = slope_x[x : x + 1] * rows_y[0:HALO_Y]
        window[at, 2 * ATOMS : 3 * ATOMS] = rows_x[x : x + 1] * slope_y[0:HALO_Y]
    entry = neighbor_ref[...]
    lows[...] = entry & 255
    highs[...] = entry >> 8
    sub = lax.broadcasted_iota(jnp.int32, (ATOMS, 2 * ATOMS), 0)

    def two_rows(ref, k):
        return jnp.concatenate([ref[pl.ds(k, 1), :], ref[pl.ds(k + 1, 1), :]], axis=1)

    def heat(pair, carry):
        hots[pair] = jnp.where(sub == two_rows(lows, 2 * pair), 1.0, 0.0).astype(BF16)
        return carry

    lax.fori_loop(0, NEIGHBORS // 2, heat, 0)
    ghosts[27] = jnp.zeros((EXPORTED + 16, 128), BF16)
    table[0, 0:CHANNELS, :] = up
    table[0, CHANNELS:ROWS, :] = spot.astype(BF16)

    pl.semaphore_wait(barrier, (NZ - 1) + (PLANES - 1) + len(LENT))

    def part_copy(c):
        l = lax.rem(gz + c, NZ)
        return pltpu.make_async_remote_copy(
            src_ref=parts_out.at[l],
            dst_ref=parts_in.at[gz],
            send_sem=parts_send.at[c],
            recv_sem=parts_recv.at[NZ - c],
            device_id=(gx, gy, l),
            device_id_type=MESH,
        )

    def part_arrival(c):
        l = lax.rem(gz + c, NZ)
        return pltpu.make_async_remote_copy(
            src_ref=parts_out.at[l],
            dst_ref=parts_in.at[l],
            send_sem=parts_send.at[c],
            recv_sem=parts_recv.at[c],
            device_id=(gx, gy, l),
            device_id_type=MESH,
        )

    def remote(source, target, send, recv, device):
        return pltpu.make_async_remote_copy(
            src_ref=source,
            dst_ref=target,
            send_sem=send,
            recv_sem=recv,
            device_id=device,
            device_id_type=MESH,
        )

    def far_copy(side):
        return remote(
            ghosts.at[13], ghosts.at[9 * (side + 1) + 4], far_send, far_recv, shifted(far, 0, 0)
        )

    def beside_copy(n):
        b, c = BESIDE[n]
        slot = 9 + 3 * (b + 1) + (c + 1)
        return remote(
            ghosts.at[13], ghosts.at[slot], beside_send.at[n], beside_recv.at[n], shifted(0, -b, -c)
        )

    def beyond_copy(n):
        b, c = BESIDE[n]
        slot = 9 * (far + 1) + 3 * (b + 1) + (c + 1)
        return remote(
            ghosts.at[9 * (far + 1) + 4],
            ghosts.at[slot],
            beyond_send.at[n],
            beyond_recv.at[n],
            shifted(0, -b, -c),
        )

    def near_copy(side):
        return remote(
            ghosts.at[pl.ds(9, 9)],
            ghosts.at[pl.ds(9 * (side + 1), 9)],
            near_send,
            near_recv,
            shifted(near, 0, 0),
        )

    far_copy(-far).start()
    for c in range(1, NZ):
        part_copy(c).start()
    for n in range(8):
        beside_copy(n).start()

    parts_in[gz] = parts_out[gz]

    for c in range(1, NZ):
        part_arrival(c).wait_recv()
    total = parts_in[0] + parts_in[1] + parts_in[2] + parts_in[3]
    planes_out[:, 0, :] = total[:, 0:128]
    planes_out[:, 1, :] = total[:, 128:256]

    def plane_copy(x, y, p):
        return pltpu.make_async_remote_copy(
            src_ref=planes_out.at[p],
            dst_ref=planes_in.at[me],
            send_sem=planes_send,
            recv_sem=planes_recv,
            device_id=(x, y, gz),
            device_id_type=MESH,
        )

    over_planes(lambda x, y, p: plane_copy(x, y, p).start())
    planes_in[me] = planes_out[me]

    for n in range(8):
        beside_copy(n).wait_recv()
    near_copy(-near).start()
    far_copy(far).wait_recv()
    for n in range(8):
        beyond_copy(n).start()
    row = lax.broadcasted_iota(jnp.int32, (16, 128), 0)
    lane = lax.broadcasted_iota(jnp.int32, (16, 128), 1)

    def enter(h):
        first = 4 * (h - 1)
        lent = jnp.concatenate([ghosts[first + q, 0:EXPORTED, :] for q in range(4)], axis=0)
        table[h, 0:CHANNELS, :] = lent.astype(F32).T.astype(BF16)
        spots = []
        for q in range(4):
            s = first + q
            a, b, c = s // 9 - 1, lax.rem(s // 3, 3) - 1, lax.rem(s, 3) - 1
            away = jnp.where(
                row == 0, a * CX, jnp.where(row == 1, b * CY, jnp.where(row == 2, c * CZ, 0))
            )
            spots.append(
                ghosts[s, EXPORTED : EXPORTED + 16, :].astype(F32) + away.astype(F32)
            )
        table[h, CHANNELS:ROWS, 0:128] = jnp.where(lane < EXPORTED, spots[0], spots[1]).astype(BF16)
        table[h, CHANNELS:ROWS, 128:256] = jnp.where(lane < EXPORTED, spots[2], spots[3]).astype(BF16)

    near_copy(near).wait_recv()
    soon, late = 4 - 3 * odd, 1 + 4 * odd

    def enter_soon(n, carry):
        enter(soon + n)
        return carry

    lax.fori_loop(0, 4, enter_soon, 0)

    def gather_soon(pair, carry):
        hot = hots[pair]
        gathered[0:ROWS, :] = dot(table[0], hot)
        gathered[ROWS : 5 * ROWS, :] = dot(
            table[pl.ds(soon, 4)].reshape(4 * ROWS, 256), hot
        )
        high8 = jnp.broadcast_to(two_rows(highs, 2 * pair), (8, 2 * ATOMS)) - soon
        for r in range(0, ROWS, 8):
            at = pl.ds(r, 8)
            result = gathered[at, :]
            for n in range(4):
                result = jnp.where(high8 == n, gathered[pl.ds(ROWS * (n + 1) + r, 8), :], result)
            partial[pair, at, :] = result
        return carry

    lax.fori_loop(0, NEIGHBORS // 2, gather_soon, 0)

    weight_high, weight_low = halves(radial_ref[...])
    weights = jnp.concatenate(
        [weight_high, weight_high, weight_low, jnp.zeros((104, CHANNELS), F32)], axis=0
    ).T[:, 0:24].astype(BF16)

    pltpu.make_async_remote_copy(
        src_ref=planes_out.at[pl.ds(0, PLANES - 1)],
        dst_ref=planes_in.at[pl.ds(0, PLANES - 1)],
        send_sem=planes_send,
        recv_sem=planes_recv,
        device_id=(gx, gy, gz),
        device_id_type=MESH,
    ).wait_recv()
    plane = [planes_in[:, 0, :], planes_in[:, 1, :]]
    spread = []
    for x, half, at in WINDOWS:
        line = jnp.zeros((NX, 128), F32)
        for j in range(NY):
            piece = plane[half][NX * j : NX * (j + 1)]
            piece = pltpu.roll(piece, (32 * j - at) % 128, 1)
            inside = jnp.logical_and(lane >= 32 * j, lane < 32 * j + HALO_Y)
            line = jnp.where(inside, piece, line)
        spread.append(line)
    spread.append(jnp.zeros((256 - NX * HALO_X, 128), F32))
    lines = jnp.concatenate(spread, axis=0)
    spectrum = dot(along_x_ref[...], dot(lines, along_yt_ref[...], HIGHEST), HIGHEST)
    mode = gz * PLANES + me
    number = jnp.where(mode <= CZ * NZ // 2, mode, mode - CZ * NZ // 2).astype(F32)
    wave = number * (2.0 * math.pi / (CZ * NZ))
    square = square_ref[...] + wave * wave
    positive = square > 0.0
    safe = jnp.where(positive, square, 1.0)
    filtered = spectrum * jnp.where(
        positive, 4.0 * math.pi * jnp.exp(-square / (4.0 * ewald_beta_sq)) / safe, 0.0
    )
    lines = dot(dot(along_xt_ref[...], filtered, HIGHEST), along_y_ref[...], HIGHEST)
    for j in range(NY):
        for half in range(2):
            piece = jnp.zeros((NX, 128), F32)
            for x, which, at in WINDOWS:
                if which == half:
                    line = pltpu.roll(lines[NX * x : NX * (x + 1)], (at - 32 * j) % 128, 1)
                    inside = jnp.logical_and(lane >= at, lane < at + HALO_Y)
                    piece = jnp.where(inside, line, piece)
            back_out[NX * j : NX * (j + 1), half, :] = piece

    def back_copy(x, y, p):
        return pltpu.make_async_remote_copy(
            src_ref=back_out.at[p],
            dst_ref=back_in.at[me],
            send_sem=back_send,
            recv_sem=back_recv,
            device_id=(x, y, gz),
            device_id_type=MESH,
        )

    over_planes(lambda x, y, p: back_copy(x, y, p).start())
    back_in[me] = back_out[me]

    for n in range(8):
        beyond_copy(n).wait_recv()

    def enter_late(n, carry):
        enter(late + n)
        return carry

    lax.fori_loop(0, 3, enter_late, 0)
    here = spot[0:8] + spot[8:16]
    count = count_ref[...]
    for a in range(4):
        sums[a] = jnp.zeros((CHANNELS, ATOMS), F32)
    centre = lax.broadcasted_iota(jnp.int32, (8, 2 * ATOMS), 0).astype(F32) * basis_step

    def gather(pair, carry):
        k = 2 * pair
        gathered[0 : 3 * ROWS, :] = dot(table[pl.ds(late, 3)].reshape(3 * ROWS, 256), hots[pair])
        high8 = jnp.broadcast_to(two_rows(highs, k), (8, 2 * ATOMS)) - late

        def chosen(start):
            result = partial[pair, pl.ds(start, 8), :]
            for n in range(3):
                result = jnp.where(high8 == n, gathered[pl.ds(start + ROWS * n, 8), :], result)
            return result

        there = chosen(CHANNELS) + chosen(CHANNELS + 8)
        rel = there - jnp.concatenate([here, here], axis=1)
        dist = jnp.sqrt(jnp.sum(rel * rel, axis=0, keepdims=True) + 1.0)
        used = jnp.concatenate([count > k, count > k + 1], axis=1).astype(F32)
        gap = (dist - centre) / basis_width
        basis = jnp.exp(-(gap * gap)) * used
        slope = basis * gap * (-2.0 / basis_width)
        basis_high, basis_low = halves(basis)
        slope_high, slope_low = halves(slope)
        radials[0:CHANNELS, :] = dot(
            weights, jnp.concatenate([basis_high, basis_low, basis_high], axis=0).astype(BF16)
        )
        radials[CHANNELS : 2 * CHANNELS, :] = dot(
            weights, jnp.concatenate([slope_high, slope_low, slope_high], axis=0).astype(BF16)
        )
        inverse = 1.0 / dist
        relatives[k] = rel[:, 0:ATOMS]
        relatives[k + 1] = rel[:, ATOMS:]
        inverses[k] = jnp.broadcast_to(inverse[:, 0:ATOMS], (8, ATOMS))
        inverses[k + 1] = jnp.broadcast_to(inverse[:, ATOMS:], (8, ATOMS))
        along = [jnp.broadcast_to(rel[a : a + 1], (8, 2 * ATOMS)) for a in range(3)]
        for c in range(0, CHANNELS, 8):
            at = pl.ds(c, 8)
            source = chosen(c)
            message = radials[at, :] * source
            turn = radials[pl.ds(CHANNELS + c, 8), :] * source
            messages[k, at, :] = message[:, 0:ATOMS]
            messages[k + 1, at, :] = message[:, ATOMS:]
            turned[k, at, :] = turn[:, 0:ATOMS]
            turned[k + 1, at, :] = turn[:, ATOMS:]
            sums[0, at, :] += message[:, 0:ATOMS] + message[:, ATOMS:]
            for a in range(3):
                moved = message * along[a]
                sums[a + 1, at, :] += moved[:, 0:ATOMS] + moved[:, ATOMS:]
        return carry

    lax.fori_loop(0, NEIGHBORS // 2, gather, 0)

    scalar = sums[0] * message_scale
    vector = [sums[a + 1] * (message_scale * vector_scale) for a in range(3)]
    invariant = scalar + scalar * scalar + (
        vector[0] * vector[0] + vector[1] * vector[1] + vector[2] * vector[2]
    )
    w_out = w_out_ref[...]
    hidden = feat.astype(F32) + dot(w_out, invariant.astype(BF16))
    wide = (
        lax.broadcasted_iota(jnp.int32, (CHANNELS, CHANNELS), 0)
        == lax.broadcasted_iota(jnp.int32, (CHANNELS, CHANNELS), 1)
    ).astype(BF16)
    readout = dot_nt(wide, jnp.broadcast_to(energy_ref[...], (16, CHANNELS)))[:, 0:1]
    gate = 1.0 / (1.0 + jnp.exp(-hidden))
    short = jnp.sum(readout * (hidden * gate), axis=0, keepdims=True)
    d_hidden = readout * (gate * (1.0 + hidden * (1.0 - gate)))
    back_high, back_low = halves(d_hidden)
    w_out_t = w_out.astype(F32).T.astype(BF16)
    d_invariant = dot(w_out_t, back_high.astype(BF16)) + dot(w_out_t, back_low.astype(BF16))
    d_invariant = d_invariant.astype(BF16).astype(F32)
    sums[0] = d_invariant * (1.0 + 2.0 * scalar) * message_scale
    for a in range(3):
        sums[a + 1] = d_invariant * vector[a] * (2.0 * message_scale * vector_scale)

    pltpu.make_async_remote_copy(
        src_ref=back_out.at[pl.ds(0, PLANES - 1)],
        dst_ref=back_in.at[pl.ds(0, PLANES - 1)],
        send_sem=back_send,
        recv_sem=back_recv,
        device_id=(gx, gy, gz),
        device_id_type=MESH,
    ).wait_recv()
    modes[gz, :, 0:128] = back_in[:, 0, :]
    modes[gz, :, 128:256] = back_in[:, 1, :]

    def mode_copy(c):
        return pltpu.make_async_remote_copy(
            src_ref=modes.at[gz],
            dst_ref=modes.at[gz],
            send_sem=modes_send.at[c],
            recv_sem=modes_recv.at[NZ - c],
            device_id=(gx, gy, lax.rem(gz + c, NZ)),
            device_id_type=MESH,
        )

    def mode_arrival(c):
        l = lax.rem(gz + c, NZ)
        return pltpu.make_async_remote_copy(
            src_ref=modes.at[gz],
            dst_ref=modes.at[l],
            send_sem=modes_send.at[c],
            recv_sem=modes_recv.at[c],
            device_id=(gx, gy, l),
            device_id_type=MESH,
        )

    for c in range(1, NZ):
        mode_copy(c).start()

    pushed[...] = jnp.zeros_like(pushed)

    def derive(pair, total):
        k = 2 * pair
        pushes = []
        for e in range(2):
            rel = relatives[k + e]
            along = [jnp.broadcast_to(rel[a : a + 1], (8, ATOMS)) for a in range(3)]
            stretch = jnp.zeros((8, ATOMS), F32)
            direct = [jnp.zeros((8, ATOMS), F32) for _ in range(3)]
            for c in range(0, CHANNELS, 8):
                at = pl.ds(c, 8)
                message = messages[k + e, at, :]
                d_message = sums[0, at, :]
                for a in range(3):
                    d_vector = sums[a + 1, at, :]
                    d_message += d_vector * along[a]
                    direct[a] += d_vector * message
                stretch += d_message * turned[k + e, at, :]
            pull = jnp.sum(stretch, axis=0, keepdims=True) * inverses[k + e][0:1]
            rows = [jnp.sum(direct[a], axis=0, keepdims=True) + pull * rel[a : a + 1] for a in range(3)]
            push = jnp.concatenate(rows + [jnp.zeros((5, ATOMS), F32)], axis=0)
            total = total + push
            pushes.append(push)
        push = jnp.concatenate(pushes, axis=1)
        high = two_rows(highs, k)
        push_high, push_low = halves(push)
        masks = [high == h for h in range(BLOCKS)]
        left = jnp.concatenate(
            [jnp.where(mask, push_high, 0.0) for mask in masks]
            + [jnp.where(mask, push_low, 0.0) for mask in masks],
            axis=0,
        ).astype(BF16)
        pushed[...] += dot_nt(left, hots[pair])
        return total

    pulled = lax.fori_loop(0, NEIGHBORS // 2, derive, jnp.zeros((8, ATOMS), F32))
    reach = pushed[0 : 8 * BLOCKS, :] + pushed[8 * BLOCKS : 16 * BLOCKS, :]
    for s, a, b, c in LENT:
        h, q = s // 4 + 1, s % 4
        piece = reach[8 * h : 8 * (h + 1), 128 * (q // 2) : 128 * (q // 2 + 1)]
        grads_out[s] = (pltpu.roll(piece, 64, 1) if q % 2 else piece)[0:4]

    def grads_copy(s, a, b, c):
        return pltpu.make_async_remote_copy(
            src_ref=grads_out.at[s],
            dst_ref=grads_in.at[s],
            send_sem=grads_send.at[s],
            recv_sem=grads_recv.at[s],
            device_id=shifted(a, b, c),
            device_id_type=MESH,
        )

    for slot in LENT:
        grads_copy(*slot).start()

    for slot in LENT:
        grads_copy(*slot).wait_recv()
    returned = grads_in[LENT[0][0]]
    for slot in LENT[1:]:
        returned = returned + grads_in[slot[0]]
    keep = jnp.where(lax.broadcasted_iota(jnp.int32, (128, ATOMS), 0) < EXPORTED, pick, 0.0)
    returned = jnp.concatenate([returned, jnp.zeros((4, 128), F32)], axis=0)
    grad = reach[0:8] - pulled + dot(returned, keep, HIGHEST)

    for c in range(1, NZ):
        mode_arrival(c).wait_recv()
    field = dot(
        jnp.concatenate([modes[l] for l in range(NZ)], axis=0), window[...], HIGHEST
    )
    here_waves = z_waves[...]
    potential = jnp.sum(here_waves * field[:, 0:ATOMS], axis=0, keepdims=True)
    along_first = jnp.sum(here_waves * field[:, ATOMS : 2 * ATOMS], axis=0, keepdims=True)
    along_second = jnp.sum(here_waves * field[:, 2 * ATOMS :], axis=0, keepdims=True)
    along_third = jnp.sum(z_slopes[...] * field[:, 0:ATOMS], axis=0, keepdims=True)
    forces_ref[0:1, :] = -(grad[0:1] + charge * along_first)
    forces_ref[1:2, :] = -(grad[1:2] + charge * along_second)
    forces_ref[2:3, :] = -(grad[2:3] + charge * along_third)
    atom_energy_ref[...] = short + 0.5 * charge * potential

    for c in range(1, NZ):
        part_copy(c).wait_send()
        mode_copy(c).wait_send()
    far_copy(-far).wait_send()
    near_copy(-near).wait_send()
    for n in range(8):
        beside_copy(n).wait_send()
        beyond_copy(n).wait_send()
    for slot in LENT:
        grads_copy(*slot).wait_send()
    pltpu.make_async_remote_copy(
        src_ref=planes_out.at[pl.ds(0, PLANES - 1)],
        dst_ref=planes_in.at[pl.ds(0, PLANES - 1)],
        send_sem=planes_send,
        recv_sem=planes_recv,
        device_id=(gx, gy, gz),
        device_id_type=MESH,
    ).wait_send()
    pltpu.make_async_remote_copy(
        src_ref=back_out.at[pl.ds(0, PLANES - 1)],
        dst_ref=back_in.at[pl.ds(0, PLANES - 1)],
        send_sem=back_send,
        recv_sem=back_recv,
        device_id=(gx, gy, gz),
        device_id_type=MESH,
    ).wait_send()


def per_device(
    atom_cell,
    atom_frac,
    features,
    ghost_export,
    neighbors,
    neighbor_count,
    w_up,
    radial_weight,
    w_out,
    energy_weight,
    charge_weight,
):
    vmem = pl.BlockSpec(memory_space=pltpu.VMEM)
    constants = tables()
    dma = pltpu.SemaphoreType.DMA
    forces, atom_energy = pl.pallas_call(
        kernel,
        name="layer",
        out_shape=(
            pltpu.VMEM((3, ATOMS), F32),
            pltpu.VMEM((1, ATOMS), F32),
        ),
        in_specs=[vmem] * (11 + len(constants)),
        out_specs=(vmem, vmem),
        scratch_shapes=[
            pltpu.VMEM((NZ, PLANES, 256), F32),
            pltpu.VMEM((NZ, PLANES, 256), F32),
            pltpu.VMEM((PLANES, 2, 128), F32),
            pltpu.VMEM((PLANES, 2, 128), F32),
            pltpu.VMEM((PLANES, 2, 128), F32),
            pltpu.VMEM((PLANES, 2, 128), F32),
            pltpu.VMEM((NZ, PLANES, 256), F32),
            pltpu.VMEM((28, EXPORTED + 16, 128), BF16),
            pltpu.VMEM((27, 4, 128), F32),
            pltpu.VMEM((27, 4, 128), F32),
            pltpu.VMEM((16, ATOMS), F32),
            pltpu.VMEM((CZ * NZ, ATOMS), F32),
            pltpu.VMEM((CZ * NZ, ATOMS), F32),
            pltpu.VMEM((256, 3 * ATOMS), F32),
            pltpu.VMEM((BLOCKS, ROWS, 256), BF16),
            pltpu.VMEM((5 * ROWS, 2 * ATOMS), F32),
            pltpu.VMEM((NEIGHBORS // 2, ROWS, 2 * ATOMS), F32),
            pltpu.VMEM((2 * CHANNELS, 2 * ATOMS), F32),
            pltpu.VMEM((NEIGHBORS, CHANNELS, ATOMS), F32),
            pltpu.VMEM((NEIGHBORS, CHANNELS, ATOMS), F32),
            pltpu.VMEM((NEIGHBORS // 2, 256, 2 * ATOMS), BF16),
            pltpu.VMEM((NEIGHBORS, ATOMS), jnp.int32),
            pltpu.VMEM((NEIGHBORS, ATOMS), jnp.int32),
            pltpu.VMEM((NEIGHBORS, 8, ATOMS), F32),
            pltpu.VMEM((NEIGHBORS, 8, ATOMS), F32),
            pltpu.VMEM((4, CHANNELS, ATOMS), F32),
            pltpu.VMEM((16 * BLOCKS, 256), F32),
            dma((NZ,)),
            dma((NZ,)),
            dma,
            dma,
            dma,
            dma,
            dma((NZ,)),
            dma((NZ,)),
            dma((8,)),
            dma((8,)),
            dma,
            dma,
            dma((8,)),
            dma((8,)),
            dma,
            dma,
            dma((27,)),
            dma((27,)),
        ],
        compiler_params=pltpu.CompilerParams(collective_id=0, has_side_effects=True),
    )(
        atom_cell,
        atom_frac,
        features,
        ghost_export.reshape(1, EXPORTED),
        neighbors.T,
        neighbor_count.reshape(1, ATOMS),
        w_up,
        radial_weight.T,
        w_out,
        energy_weight.reshape(1, CHANNELS),
        charge_weight.reshape(1, CHANNELS),
        *constants,
    )
    return forces, atom_energy.reshape(ATOMS)


def solution(mesh):
    whole = ("gx", "gy", "gz")
    in_specs = (
        P(None, whole),
        P(None, whole),
        P(None, whole),
        P(whole),
        P(whole, None),
        P(whole),
        P(),
        P(),
        P(),
        P(),
        P(),
    )
    out_specs = (P(None, whole), P(whole))
    return jax.shard_map(
        per_device, mesh=mesh, in_specs=in_specs, out_specs=out_specs, check_vma=False
    )
```
